32 devices in a mesh: seq: 4 (over y, x), dp: 8 (over z, core).
Axes of the slice: x: 2, y: 2, z: 4, core: 2. Of those that a mesh axis runs over, the one named last changes fastest.
Arguments:
- tokens: bfloat16 [8, 1024, 2304], P('dp', 'seq'), may hold values from -6 to 6
- cotangent: bfloat16 [8, 1024, 2304], P('dp', 'seq'), may hold values from -6 to 6
- qkv_weight: float32 [256, 9, 4096], P(('seq', 'dp')), may hold values from -0.125 to 0.125
- out_weight: float32 [256, 8, 2304], P(('seq', 'dp')), may hold values from -0.125 to 0.125
- geglu_weight: float32 [256, 9, 18432], P(('seq', 'dp')), may hold values from -0.125 to 0.125
- down_weight: float32 [256, 36, 2304], P(('seq', 'dp')), may hold values from -0.0625 to 0.0625
- norm_gains: float32 [2304, 4], P(('seq', 'dp')), may hold values from 0.5 to 1.5
- seq_lengths: int32 [8], P('dp'), may hold values from 129 to 1024, as said below
- prefix_lengths: int32 [8], P('dp'), may hold values from 0 to 256, as said below
- block_owners: int32 [1188], replicated, may hold values from 0 to 31, as said below
- first_moment: float32 [1216, 256, 256], P(('seq', 'dp')), may hold values from -0.0068359375 to 0.0068359375
- second_moment: float32 [1216, 256, 256], P(('seq', 'dp')), may hold values from 8e-07 to 3.2e-06
- left_basis: float32 [1216, 256, 256], P(('seq', 'dp')), may hold values from -0.375 to 0.375
- right_basis: float32 [1216, 256, 256], P(('seq', 'dp')), may hold values from -0.375 to 0.375
- slot_weight: float32 [1216, 256, 256], P(('seq', 'dp')), may hold values from -1.5 to 1.5
Outputs:
- layer_out: bfloat16 [8, 1024, 2304], P('dp', 'seq')
- row_rms: float32 [8, 1024], P('dp', 'seq')
- token_grad: float32 [8, 1024, 2304], P('dp', 'seq')
- qkv_grad: float32 [256, 9, 4096], P(('seq', 'dp'))
- out_grad: float32 [256, 8, 2304], P(('seq', 'dp'))
- geglu_grad: float32 [256, 9, 18432], P(('seq', 'dp'))
- down_grad: float32 [256, 36, 2304], P(('seq', 'dp'))
- gains_grad: float32 [2304, 4], P(('seq', 'dp'))
- first_new: float32 [1216, 256, 256], P(('seq', 'dp'))
- second_new: float32 [1216, 256, 256], P(('seq', 'dp'))
- weight_new: float32 [1216, 256, 256], P(('seq', 'dp'))
The draws below stay inside these ranges and needn't reach their ends.
Inputs may be any that keep to these rules, and one draw needn't show every extreme that they name: `seq_lengths`: one sequence is full, with length 1024. `prefix_lengths`: each prefix is at most its sequence's length; the full sequence's prefix is 256. `block_owners`: each owner is listed for at most 38 blocks, and some owner for exactly 38.
All inputs are finite; a program needn't handle non-finite values.
Results may differ from the reference program's by a relative error of at most 0.017.
Values may be sent and summed in bfloat16 or wider, within the bound.
A program may use at most 512 MiB of HBM per device.

```python
import math
import jax
import jax.numpy as jnp
from jax import lax

D = 2304
QUERY_HEADS = 8
KV_HEAD_COUNT = 4
HEAD_SIZE = 256
FF = 9216
BLK = 256
TOK_DEV = 256
TOKEN_SLOTS = 1024
SEQS = 8
QUERY_FEATURES = 2048
KEY_FEATURES = 1024
NB = 1188
CAP = 38
OWNER_SLOTS = 1216
N_SEQ = 4
N_DP = 8


def lengths_and_prefix(key):
    base = jax.random.fold_in(key, 11)
    key_one, key_two, key_three = jax.random.split(base, 3)
    lengths = jax.random.randint(key_one, (SEQS,), TOKEN_SLOTS // 8 + 1, TOKEN_SLOTS + 1)
    chosen = jax.random.randint(key_two, (), 0, SEQS)
    marker = jnp.arange(SEQS) == chosen
    lengths = jnp.where(marker, TOKEN_SLOTS, lengths)
    ceiling = jnp.minimum(lengths, TOK_DEV)
    prefixes = jax.random.randint(key_three, (SEQS,), 0, ceiling + 1)
    prefixes = jnp.where(marker, TOK_DEV, prefixes)
    return (lengths.astype(jnp.int32), prefixes.astype(jnp.int32))


def draw_seq_lengths(key, part):
    return lengths_and_prefix(key)[0]


def draw_prefix_lengths(key, part):
    return lengths_and_prefix(key)[1]


def draw_block_owners(key, part):
    key_one, key_two = jax.random.split(jax.random.fold_in(key, 23))
    order = jax.random.permutation(key_one, NB)
    offset = jax.random.randint(key_two, (), 0, N_SEQ * N_DP)
    return ((order + offset) % (N_SEQ * N_DP)).astype(jnp.int32)


def block_scale(key, shape, cuts, low, largest):
    level = 1.0
    for axis_at, shards_of in cuts:
        draws = jax.random.uniform(jax.random.fold_in(jax.random.fold_in(key, 6), axis_at), (shards_of,), jnp.float32, low / len(cuts), largest / len(cuts))
        level = level * jnp.repeat(jnp.exp(draws), shape[axis_at] // shards_of).reshape((-1,) + (1,) * (len(shape) - 1 - axis_at))
    return level


def noise(own_key, extent, scale, most, cuts=(), kind=jnp.bfloat16):
    level = block_scale(own_key, extent, cuts, -0.22, 0.18) if cuts else 1.0
    values = jax.random.normal(own_key, extent, jnp.float32) * scale * level
    return jnp.minimum(jnp.maximum(values, -most), most).astype(kind)


def setup_inputs(seed: int = 0) -> dict:
    arg_keys = jax.random.split(jax.random.key(seed), 16)
    return {
        "tokens": noise(arg_keys[0], (SEQS, TOKEN_SLOTS, D), 1.0, 6.0, ((0, 8), (1, 4))),
        "cotangent": noise(arg_keys[1], (SEQS, TOKEN_SLOTS, D), 1.0, 6.0, ((0, 8), (1, 4))),
        "qkv_weight": noise(arg_keys[2], (BLK, D // BLK, QUERY_FEATURES + 2 * KEY_FEATURES), D ** -0.5, 0.125, ((0, 32),), jnp.float32),
        "out_weight": noise(arg_keys[3], (BLK, QUERY_FEATURES // BLK, D), QUERY_FEATURES ** -0.5, 0.125, ((0, 32),), jnp.float32),
        "geglu_weight": noise(arg_keys[4], (BLK, D // BLK, 2 * FF), D ** -0.5, 0.125, ((0, 32),), jnp.float32),
        "down_weight": noise(arg_keys[5], (BLK, FF // BLK, D), FF ** -0.5, 0.0625, ((0, 32),), jnp.float32),
        "norm_gains": jnp.clip(1.0 + 0.1 * jax.random.normal(arg_keys[6], (D, 4), jnp.float32), 0.5, 1.5),
        "seq_lengths": draw_seq_lengths(jax.random.fold_in(arg_keys[15], 71), 0),
        "prefix_lengths": draw_prefix_lengths(jax.random.fold_in(arg_keys[15], 71), 0),
        "block_owners": draw_block_owners(jax.random.fold_in(arg_keys[15], 71), 0),
        "first_moment": noise(arg_keys[10], (OWNER_SLOTS, BLK, BLK), 0.00044, 0.0068359375, ((0, 32),), jnp.float32),
        "second_moment": jnp.clip(jnp.exp(math.log(3.2000000373955118e-06) - 1.3862944 * jax.random.uniform(arg_keys[11], (OWNER_SLOTS, BLK, BLK), jnp.float32) ** block_scale(arg_keys[11], (OWNER_SLOTS, BLK, BLK), ((0, 32),), -0.2, 0.2)), 8.000000093488779e-07, 3.2000000373955118e-06),
        "left_basis": noise(arg_keys[12], (OWNER_SLOTS, BLK, BLK), BLK ** -0.5, 0.375, ((0, 32),), jnp.float32),
        "right_basis": noise(arg_keys[13], (OWNER_SLOTS, BLK, BLK), BLK ** -0.5, 0.375, ((0, 32),), jnp.float32),
        "slot_weight": noise(arg_keys[14], (OWNER_SLOTS, BLK, BLK), 0.1, 1.5, ((0, 32),), jnp.float32),
    }


@jax.custom_vjp
def low(v):
    return lax.optimization_barrier(v.astype(jnp.bfloat16)).astype(jnp.float32)

@jax.custom_vjp
def low_back(v):
    return v

def low_keep(v):
    return (low(v), None)

def low_pass(kept, grad):
    return (grad,)

def back_keep(v):
    return (v, None)

def back_low(kept, grad):
    return (low(grad),)
low.defvjp(low_keep, low_pass)
low_back.defvjp(back_keep, back_low)
EPSILON = 1e-06
SOFT_CAP = 50.0
NEGATIVE = -1e+30
BETA_ONE = 0.9
BETA_TWO = 0.95
STEP_RATE = 0.05
TINY_ADD = 1e-08
CLIP_NORM = 1.0

def as_matrix(weight):
    return jnp.transpose(weight, (1, 0, 2)).reshape(weight.shape[0] * weight.shape[1], weight.shape[2])

def matmul(left, right):
    return jnp.dot(left, right, precision=lax.Precision.HIGHEST, preferred_element_type=jnp.float32)

def rms_norm(value_rows, gain):
    inverse = lax.rsqrt(lax.optimization_barrier(jnp.mean(value_rows * value_rows, axis=-1, keepdims=True)) + EPSILON)
    return value_rows * inverse * gain

def layer(params, inputs, length, prefix):
    qkv_weight, out_weight, geglu_weight, down_weight, norm_gains = params
    gains = low(norm_gains)
    head_group = QUERY_HEADS // KV_HEAD_COUNT
    normed = low(rms_norm(inputs, gains[:, 0]))
    merged_heads = low(low_back(matmul(normed, low(as_matrix(qkv_weight)))))
    query_rows = merged_heads[:, :QUERY_FEATURES].reshape(TOKEN_SLOTS, KV_HEAD_COUNT, head_group, HEAD_SIZE)
    key_rows = merged_heads[:, QUERY_FEATURES:QUERY_FEATURES + KEY_FEATURES].reshape(TOKEN_SLOTS, KV_HEAD_COUNT, HEAD_SIZE)
    value_rows = merged_heads[:, QUERY_FEATURES + KEY_FEATURES:].reshape(TOKEN_SLOTS, KV_HEAD_COUNT, HEAD_SIZE)
    raw = low_back(jnp.einsum('igrh,jgh->grij', query_rows, key_rows, precision=lax.Precision.HIGHEST))
    capped = SOFT_CAP * jnp.tanh(raw * HEAD_SIZE ** (-0.5) / SOFT_CAP)
    position = jnp.arange(TOKEN_SLOTS, dtype=jnp.int32)
    visible = (position[None, :] < length) & ((position[None, :] <= position[:, None]) | (position[None, :] < prefix))
    scores = jnp.where(visible, capped, NEGATIVE)
    highest = lax.optimization_barrier(jnp.max(scores, axis=-1, keepdims=True))
    exponent = jnp.exp(scores - highest)
    probs = low(exponent / lax.optimization_barrier(jnp.sum(exponent, axis=-1, keepdims=True)))
    mixed = jnp.einsum('grij,jgh->igrh', probs, value_rows, precision=lax.Precision.HIGHEST).reshape(TOKEN_SLOTS, QUERY_FEATURES)
    mixed = low(low_back(mixed))
    attended = low_back(matmul(mixed, low(as_matrix(out_weight))))
    hidden = inputs + rms_norm(attended, gains[:, 1])
    ffn_in = low(rms_norm(hidden, gains[:, 2]))
    gate_up = low_back(matmul(ffn_in, low(as_matrix(geglu_weight))))
    product = low(jax.nn.gelu(gate_up[:, :FF], approximate=True) * gate_up[:, FF:])
    branch = low_back(matmul(product, low(as_matrix(down_weight))))
    output = hidden + rms_norm(branch, gains[:, 3])
    live = (position < length).astype(jnp.float32)[:, None]
    return output * live

def owner_slots(owners, capacity):
    devices = N_SEQ * N_DP
    onehot = (owners[:, None] == jnp.arange(devices, dtype=jnp.int32)[None, :]).astype(jnp.int32)
    before = jnp.cumsum(onehot, axis=0) - onehot
    rank = lax.optimization_barrier(jnp.sum(before * onehot, axis=1))
    return (owners * capacity + rank).astype(jnp.int32)

def to_blocks(gradient):
    count_of_rows, groups, col_count = gradient.shape
    shaped = gradient.reshape(count_of_rows, groups, col_count // BLK, BLK)
    return jnp.transpose(shaped, (1, 2, 0, 3)).reshape(-1, count_of_rows, BLK)

def soap_slot(item):
    gradient, first, second, left, right, master = item
    size = jnp.sqrt(jnp.sum(gradient * gradient))
    clipped = gradient * (CLIP_NORM / jnp.maximum(size, CLIP_NORM))
    rotated = matmul(matmul(left.T, clipped), right)
    first_next = BETA_ONE * first + (1.0 - BETA_ONE) * rotated
    second_next = BETA_TWO * second + (1.0 - BETA_TWO) * rotated * rotated
    direction = first_next / (jnp.sqrt(second_next) + TINY_ADD)
    update = -STEP_RATE * matmul(matmul(left, direction), right.T)
    return (first_next, second_next, master + update)

def reference(tokens, cotangent, qkv_weight, out_weight, geglu_weight, down_weight, norm_gains, seq_lengths, prefix_lengths, block_owners, first_moment, second_moment, left_basis, right_basis, slot_weight):
    params = (qkv_weight, out_weight, geglu_weight, down_weight, norm_gains)

    def one_sequence(carry, item):
        inputs, upstream, length, prefix = item
        inputs = inputs.astype(jnp.float32)

        def forward(weights, acts):
            return layer(weights, acts, length, prefix)
        output, pullback = jax.vjp(forward, params, inputs)
        weight_grads, input_grad = pullback(upstream.astype(jnp.float32))
        carry = jax.tree.map(lambda total, term: total + term, carry, weight_grads)
        rms_values = jnp.sqrt(lax.optimization_barrier(jnp.mean(inputs * inputs, axis=-1)) + EPSILON)
        return (carry, (output.astype(jnp.bfloat16), rms_values, input_grad))
    start_grads = jax.tree.map(jnp.zeros_like, params)
    grads, (layer_out, row_rms, token_grad) = lax.scan(one_sequence, start_grads, (tokens, cotangent, seq_lengths, prefix_lengths))
    qkv_grad, out_grad, geglu_grad, down_grad, gains_grad = grads
    blocks = jnp.concatenate([to_blocks(qkv_grad), to_blocks(out_grad), to_blocks(geglu_grad), to_blocks(down_grad)], axis=0)
    slots = owner_slots(block_owners, CAP)
    slotted = jnp.zeros((OWNER_SLOTS, BLK, BLK), jnp.float32).at[slots].set(blocks)
    first_new, second_new, weight_new = lax.map(soap_slot, (slotted, first_moment, second_moment, left_basis, right_basis, slot_weight))
    return (layer_out, row_rms, token_grad, qkv_grad, out_grad, geglu_grad, down_grad, gains_grad, first_new, second_new, weight_new)
```

```python
import functools

import jax
import jax.numpy as jnp
from jax import lax
from jax.experimental import pallas as pl
from jax.experimental.pallas import tpu as pltpu
from jax.sharding import PartitionSpec as P

D = 2304
QUERY_HEADS = 8
KV_HEAD_COUNT = 4
HEAD_SIZE = 256
FF = 9216
BLK = 256
QUERY_FEATURES = 2048
KEY_FEATURES = 1024


EPSILON = 1e-06
SOFT_CAP = 50.0
NEGATIVE = -1e30
BETA_ONE = 0.9
BETA_TWO = 0.95
STEP_RATE = 0.05
TINY_ADD = 1e-08
CLIP_NORM = 1.0

F32 = jnp.float32
BF16 = jnp.bfloat16
ALL = ("seq", "dp")


def norm_forward(value_rows, gain):
    inverse = lax.rsqrt(jnp.mean(value_rows * value_rows, axis=-1, keepdims=True) + EPSILON)
    return (value_rows * inverse * gain, inverse)


def norm_backward(value_rows, inverse, gain, upstream):
    weighted = upstream * gain
    cubed = inverse * inverse * inverse
    grad_in = inverse * weighted - value_rows * cubed * jnp.mean(
        value_rows * weighted, axis=-1, keepdims=True
    )
    return (grad_in, jnp.sum(upstream * value_rows * inverse, axis=0))


def dot(left, right):
    return jnp.dot(left, right, preferred_element_type=F32)


def dot_nt(left, right):
    return lax.dot_general(left, right, (((1,), (1,)), ((), ())), preferred_element_type=F32)


def dot_tn(left, right):
    return lax.dot_general(left, right, (((0,), (0,)), ((), ())), preferred_element_type=F32)


def block_probs(query, keys, row_start, length, prefix):
    raw = dot_nt(query, keys)
    bent = jnp.tanh(raw * (HEAD_SIZE ** (-0.5) / SOFT_CAP))
    key_pos = lax.broadcasted_iota(jnp.int32, raw.shape, 1)
    query_pos = row_start + lax.broadcasted_iota(jnp.int32, raw.shape, 0)
    visible = (key_pos < length) & ((key_pos <= query_pos) | (key_pos < prefix))
    capped = jnp.where(visible, SOFT_CAP * bent, NEGATIVE)
    exponent = jnp.exp(capped - jnp.max(capped, axis=-1, keepdims=True))
    prob = exponent / jnp.sum(exponent, axis=-1, keepdims=True)
    return (prob, bent)


def attention_forward_kernel(heads, length_ref, prefix_ref, merged_ref, mixed_ref):
    length, prefix = length_ref[0], prefix_ref[0]
    key_col, value_col = heads * HEAD_SIZE, (heads + 1) * HEAD_SIZE
    tokens = merged_ref.shape[0]
    for head in range(heads):
        for start in range(0, tokens, BLK):
            rows, width = slice(start, start + BLK), start + BLK
            head_cols = slice(head * HEAD_SIZE, (head + 1) * HEAD_SIZE)
            keys = merged_ref[:width, key_col : key_col + HEAD_SIZE]
            values = merged_ref[:width, value_col : value_col + HEAD_SIZE]
            prob, _ = block_probs(merged_ref[rows, head_cols], keys, start, length, prefix)
            mixed_ref[rows, head_cols] = dot(prob.astype(BF16), values).astype(BF16)


def attention_backward_kernel(
    heads, length_ref, prefix_ref, merged_ref, upstream_ref, grad_ref, keys_acc, values_acc
):
    length, prefix = length_ref[0], prefix_ref[0]
    key_col, value_col = heads * HEAD_SIZE, (heads + 1) * HEAD_SIZE
    tokens = merged_ref.shape[0]
    keys_acc[...] = jnp.zeros_like(keys_acc)
    values_acc[...] = jnp.zeros_like(values_acc)
    for head in range(heads):
        for start in range(0, tokens, BLK):
            rows, width = slice(start, start + BLK), start + BLK
            head_cols = slice(head * HEAD_SIZE, (head + 1) * HEAD_SIZE)
            query = merged_ref[rows, head_cols]
            keys = merged_ref[:width, key_col : key_col + HEAD_SIZE]
            values = merged_ref[:width, value_col : value_col + HEAD_SIZE]
            upstream = upstream_ref[rows, head_cols]
            prob, bent = block_probs(query, keys, start, length, prefix)
            grad_prob = dot_nt(upstream, values)
            balance = jnp.sum(prob * grad_prob, axis=-1, keepdims=True)
            grad_raw = (
                prob * (grad_prob - balance) * (1.0 - bent * bent) * HEAD_SIZE ** (-0.5)
            ).astype(BF16)
            grad_ref[rows, head_cols] = dot(grad_raw, keys).astype(BF16)
            keys_acc[:width, :] += dot_tn(grad_raw, query)
            values_acc[:width, :] += dot_tn(prob.astype(BF16), upstream)
    grad_ref[:, key_col : key_col + HEAD_SIZE] = keys_acc[...].astype(BF16)
    grad_ref[:, value_col : value_col + HEAD_SIZE] = values_acc[...].astype(BF16)


SMEM_SPEC = pl.BlockSpec(memory_space=pltpu.SMEM)
VMEM_SPEC = pl.BlockSpec(memory_space=pltpu.VMEM)


def attention_forward(merged, length, prefix, heads):
    tokens = merged.shape[0]
    flops = 4 * heads * tokens * tokens * HEAD_SIZE
    return pl.pallas_call(
        functools.partial(attention_forward_kernel, heads),
        out_shape=jax.ShapeDtypeStruct((tokens, heads * HEAD_SIZE), BF16),
        in_specs=[SMEM_SPEC, SMEM_SPEC, VMEM_SPEC],
        out_specs=VMEM_SPEC,
        compiler_params=pltpu.CompilerParams(vmem_limit_bytes=40 << 20),
        cost_estimate=pl.CostEstimate(
            flops=flops, bytes_accessed=4 << 20, transcendentals=2 * heads * tokens * tokens
        ),
    )(length, prefix, merged)


def attention_backward(merged, upstream, length, prefix, heads):
    tokens = merged.shape[0]
    flops = 10 * heads * tokens * tokens * HEAD_SIZE
    return pl.pallas_call(
        functools.partial(attention_backward_kernel, heads),
        out_shape=jax.ShapeDtypeStruct(merged.shape, BF16),
        in_specs=[SMEM_SPEC, SMEM_SPEC, VMEM_SPEC, VMEM_SPEC],
        out_specs=VMEM_SPEC,
        scratch_shapes=[pltpu.VMEM((tokens, HEAD_SIZE), F32), pltpu.VMEM((tokens, HEAD_SIZE), F32)],
        compiler_params=pltpu.CompilerParams(vmem_limit_bytes=48 << 20),
        cost_estimate=pl.CostEstimate(
            flops=flops, bytes_accessed=6 << 20, transcendentals=2 * heads * tokens * tokens
        ),
    )(length, prefix, merged, upstream)


def place_kernel(layout, devices, stride, slots_ref, *refs):
    pieces, extra, out = refs[: len(layout)], refs[len(layout)], refs[len(layout) + 1]
    out[...] = jnp.zeros_like(out)

    @pl.loop(0, devices)
    def _(at):
        out[at * stride + stride - 1] = extra[at]

    seq_index = slots_ref[slots_ref.shape[0] - 1]
    for piece, (turn, base, per_row, columns) in zip(pieces, layout):
        source = jnp.bitwise_xor(seq_index, turn)

        @pl.loop(0, piece.shape[0])
        def _(a, piece=piece, base=base, per_row=per_row, columns=columns, source=source):
            for local, (fixed, factor, row_factor) in enumerate(columns):
                block = base + (a + source * row_factor) * per_row + fixed + source * factor
                out[slots_ref[block]] = piece[a, :, local * BLK : (local + 1) * BLK]


def place_pieces(pieces, extra, slots, seq_index, layout, devices, stride):
    share = extra.shape[1]
    table = jnp.concatenate([slots, seq_index[None]]).astype(jnp.int32)
    return pl.pallas_call(
        functools.partial(place_kernel, layout, devices, stride),
        out_shape=jax.ShapeDtypeStruct((devices * stride, share, BLK), BF16),
        in_specs=[SMEM_SPEC] + [VMEM_SPEC] * (len(pieces) + 1),
        out_specs=VMEM_SPEC,
        compiler_params=pltpu.CompilerParams(vmem_limit_bytes=48 << 20),
        cost_estimate=pl.CostEstimate(flops=0, bytes_accessed=12 << 20, transcendentals=0),
    )(table, *pieces, extra)


def soap_kernel(
    group, incoming, first, second, left, right, master, first_out, second_out, weight_out
):
    for at in range(group):
        if len(incoming.shape) == 4:
            grad = incoming[:, at].astype(F32).reshape(BLK, BLK)
        else:
            grad = incoming[at].astype(F32)
        size = jnp.sqrt(jnp.sum(grad * grad))
        scale = CLIP_NORM / jnp.maximum(size, CLIP_NORM)
        left_low = left[at].astype(BF16)
        right_low = right[at].astype(BF16)
        turned = dot_tn(left_low, grad.astype(BF16)).astype(BF16)
        rotated = dot(turned, right_low) * scale
        first_new = BETA_ONE * first[at] + (1.0 - BETA_ONE) * rotated
        second_new = BETA_TWO * second[at] + (1.0 - BETA_TWO) * rotated * rotated
        first_out[at] = first_new
        second_out[at] = second_new
        direction = (first_new / (jnp.sqrt(second_new) + TINY_ADD)).astype(BF16)
        back_left = dot(left_low, direction).astype(BF16)
        weight_out[at] = master[at] - STEP_RATE * dot_nt(back_left, right_low)


def soap(incoming, first, second, left, right, master):
    capacity = first.shape[0]
    group = 2 if capacity % 2 == 0 else 1
    spec = pl.BlockSpec((group, BLK, BLK), lambda at: (at, 0, 0))
    if incoming.ndim == 4:
        grad_spec = pl.BlockSpec(
            (incoming.shape[0], group) + incoming.shape[2:], lambda at: (0, at, 0, 0)
        )
    else:
        grad_spec = spec
    shape = jax.ShapeDtypeStruct(first.shape, F32)
    return pl.pallas_call(
        functools.partial(soap_kernel, group),
        grid=(capacity // group,),
        out_shape=(shape, shape, shape),
        in_specs=[grad_spec] + [spec] * 5,
        out_specs=(spec, spec, spec),
        compiler_params=pltpu.CompilerParams(vmem_limit_bytes=48 << 20),
        cost_estimate=pl.CostEstimate(
            flops=8 * capacity * BLK**3,
            bytes_accessed=34 * capacity * BLK * BLK,
            transcendentals=2 * capacity * BLK * BLK,
        ),
    )(incoming, first, second, left, right, master)


def body(
    tokens,
    cotangent,
    qkv_weight,
    out_weight,
    geglu_weight,
    down_weight,
    norm_gains,
    seq_lengths,
    prefix_lengths,
    block_owners,
    first_moment,
    second_moment,
    left_basis,
    right_basis,
    slot_weight,
):
    inputs = tokens[0].astype(F32)
    upstream = cotangent[0].astype(F32)
    rows = inputs.shape[0]
    seq_count = lax.axis_size("seq")
    dp_count = lax.axis_size("dp")
    seq_index = lax.axis_index("seq")
    share = qkv_weight.shape[0]
    total_rows = rows * seq_count
    heads = QUERY_HEADS // seq_count
    query_slice = heads * HEAD_SIZE
    key_slice = KEY_FEATURES // seq_count
    ff_slice = FF // seq_count
    d_groups = D // BLK
    half = ff_slice // 2

    def swap(value, turn):
        return lax.ppermute(value, "seq", [(at, at ^ turn) for at in range(seq_count)])

    def owner_of(turn):
        return jnp.bitwise_xor(seq_index, turn)

    def pick(value, index, size, axis):
        return lax.dynamic_slice_in_dim(value, index * size, size, axis)

    def assemble(items):
        size = items[0].shape[0]
        buffer = jnp.zeros((size * seq_count,) + items[0].shape[1:], items[0].dtype)
        for turn, item in enumerate(items):
            start = (owner_of(turn) * size,) + (0,) * (item.ndim - 1)
            buffer = lax.dynamic_update_slice(buffer, item, start)
        return buffer

    def gather_rows(value):
        received = {turn: swap(value, turn) for turn in range(seq_count - 1, 0, -1)}
        return assemble([value] + [received[turn] for turn in range(1, seq_count)])

    def scatter_rows(part_of):
        received = []
        for turn in range(seq_count - 1, 0, -1):
            received.append(swap(part_of(owner_of(turn)).astype(BF16), turn))
        result = part_of(seq_index)
        for value in received:
            result = result + value.astype(F32)
        return result

    def spread(piece_for):
        received = [piece_for(seq_index)]
        for turn in range(1, seq_count):
            received.append(swap(piece_for(owner_of(turn)), turn))
        return lax.all_gather(assemble(received), "dp", axis=0, tiled=True)

    def collect(gradient):
        summed = lax.psum_scatter(gradient.astype(BF16), "dp", scatter_dimension=0, tiled=True)
        size = summed.shape[0] // seq_count
        result = [pick(summed, seq_index, size, 0)]
        for turn in range(1, seq_count):
            result.append(swap(pick(summed, owner_of(turn), size, 0), turn))
        return result

    def row_order(groups):
        at = jnp.arange(groups * BLK, dtype=jnp.int32)
        inner = at % share
        group = (at // share) % groups
        device = at // (share * groups)
        natural = share * (dp_count * (device % seq_count) + device // seq_count) + inner
        return group * BLK + natural

    def order_matrix(groups):
        return (jnp.arange(groups * BLK, dtype=jnp.int32)[:, None] == row_order(groups)[None, :]).astype(BF16)

    wide_order = order_matrix(d_groups)
    head_order = order_matrix(heads)

    def local_rows(weight):
        return jnp.transpose(weight.astype(BF16), (1, 0, 2))

    qkv_low = local_rows(qkv_weight).reshape(d_groups * share, -1)
    out_low = local_rows(out_weight)
    down_low = local_rows(down_weight)
    gain_full = lax.all_gather(norm_gains.astype(BF16), ALL, axis=0, tiled=True)

    def qkv_piece(target):
        return jnp.concatenate(
            [
                pick(qkv_low[:, :QUERY_FEATURES], target, query_slice, 1),
                pick(qkv_low[:, QUERY_FEATURES : QUERY_FEATURES + KEY_FEATURES], target, key_slice, 1),
                pick(qkv_low[:, QUERY_FEATURES + KEY_FEATURES :], target, key_slice, 1),
            ],
            axis=1,
        )

    def out_piece(target):
        return pick(out_low, target, heads, 0).reshape(heads * share, D)

    def down_piece(target):
        return pick(down_low, target, d_groups, 0).reshape(d_groups * share, D)

    qkv_slice_full = spread(qkv_piece)
    out_slice_full = spread(out_piece)

    geglu_rows = jnp.transpose(
        geglu_weight.astype(BF16).reshape(share, d_groups, 2 * seq_count, ff_slice), (2, 1, 0, 3)
    ).reshape(2 * seq_count * d_groups * share, ff_slice)
    geglu_turned = dot(geglu_rows, wide_order).astype(BF16).reshape(
        2 * seq_count, d_groups * share, ff_slice
    )

    def geglu_piece(part):
        cols = slice(part * half, (part + 1) * half)

        def piece(target):
            return jnp.concatenate(
                [
                    lax.dynamic_index_in_dim(geglu_turned, target, 0, False)[:, cols],
                    lax.dynamic_index_in_dim(geglu_turned, target + seq_count, 0, False)[:, cols],
                ],
                axis=1,
            )

        return piece

    geglu_zero = spread(geglu_piece(0))
    down_full = spread(down_piece)
    geglu_one = spread(geglu_piece(1))
    geglu_parts = (geglu_zero, geglu_one)

    gains = gain_full.astype(F32)
    normed, inverse_one = norm_forward(inputs, gains[:, 0])
    normed_turned = dot(normed.astype(BF16), wide_order).astype(BF16)
    normed_all = gather_rows(normed_turned)
    merged = dot(normed_all, qkv_slice_full).astype(BF16)
    mixed = attention_forward(merged, seq_lengths, prefix_lengths, heads)
    mixed_turned = dot(mixed, head_order).astype(BF16)
    attended = scatter_rows(lambda owner: dot(pick(mixed_turned, owner, rows, 0), out_slice_full))
    attn_normed, inverse_two = norm_forward(attended, gains[:, 1])
    hidden = inputs + attn_normed
    ffn_normed, inverse_three = norm_forward(hidden, gains[:, 2])
    ffn_turned = dot(ffn_normed.astype(BF16), wide_order).astype(BF16)
    ffn_all = gather_rows(ffn_turned)

    gates, uppers, products = [], [], []
    for part in range(2):
        gate_up = dot(ffn_all, geglu_parts[part])
        gate, upper = gate_up[:, :half], gate_up[:, half:]
        gates.append(gate)
        uppers.append(upper)
        products.append((jax.nn.gelu(gate, approximate=True) * upper).astype(BF16))

    branch_zero = dot(products[0], down_full[:half])

    def branch_part(owner):
        return pick(branch_zero, owner, rows, 0) + dot(
            pick(products[1], owner, rows, 0), down_full[half:]
        )

    branch = scatter_rows(branch_part)
    branch_normed, inverse_four = norm_forward(branch, gains[:, 3])
    query_pos = seq_index * rows + jnp.arange(rows, dtype=jnp.int32)
    live_rows = (query_pos < seq_lengths[0]).astype(F32)[:, None]
    layer_out = ((hidden + branch_normed) * live_rows).astype(BF16)
    row_rms = jnp.sqrt(jnp.mean(inputs * inputs, axis=-1) + EPSILON)

    upstream = upstream * live_rows
    grad_branch, gain_four = norm_backward(branch, inverse_four, gains[:, 3], upstream)
    branch_all = gather_rows(grad_branch.astype(BF16))
    down_sums = collect(
        jnp.concatenate([dot_tn(products[0], branch_all), dot_tn(products[1], branch_all)], axis=0)
    )
    gate_up_grads = []
    geglu_sums = []
    for part in range(2):
        grad_product = dot_nt(branch_all, down_full[part * half : (part + 1) * half])
        activated, gelu_pull = jax.vjp(lambda value: jax.nn.gelu(value, approximate=True), gates[part])
        grad_gate = gelu_pull(grad_product * uppers[part])[0]
        grad_upper = grad_product * activated
        gate_up_grad = jnp.concatenate([grad_gate, grad_upper], axis=1).astype(BF16)
        gate_up_grads.append(gate_up_grad)
        geglu_sums.append(collect(dot_tn(ffn_all, gate_up_grad)))

    def ffn_part(owner):
        return dot_nt(pick(gate_up_grads[0], owner, rows, 0), geglu_zero) + dot_nt(
            pick(gate_up_grads[1], owner, rows, 0), geglu_one
        )

    grad_ffn = dot_nt(scatter_rows(ffn_part).astype(BF16), wide_order)
    grad_hidden_norm, gain_three = norm_backward(hidden, inverse_three, gains[:, 2], grad_ffn)
    grad_hidden = upstream + grad_hidden_norm
    grad_attended, gain_two = norm_backward(attended, inverse_two, gains[:, 1], grad_hidden)
    attended_all = gather_rows(grad_attended.astype(BF16))
    grad_mixed_turned = dot_nt(attended_all, out_slice_full).astype(BF16)
    grad_mixed = dot_nt(grad_mixed_turned, head_order).astype(BF16)
    out_sums = collect(dot_tn(mixed_turned, attended_all))
    grad_merged = attention_backward(merged, grad_mixed, seq_lengths, prefix_lengths, heads)
    qkv_sums = collect(dot_tn(normed_all, grad_merged))
    grad_normed = dot_nt(
        scatter_rows(lambda owner: dot_nt(pick(grad_merged, owner, rows, 0), qkv_slice_full)).astype(BF16),
        wide_order,
    )
    grad_input_norm, gain_one = norm_backward(inputs, inverse_one, gains[:, 0], grad_normed)
    token_grad = grad_hidden + grad_input_norm

    turned = jnp.concatenate(
        [
            jnp.concatenate(
                [geglu_sums[0][turn][:, side * half : (side + 1) * half],
                 geglu_sums[1][turn][:, side * half : (side + 1) * half]],
                axis=1,
            )
            for turn in range(seq_count)
            for side in range(2)
        ],
        axis=0,
    )
    geglu_natural = dot_nt(turned, wide_order).astype(BF16).reshape(
        seq_count, 2, d_groups, share, ff_slice
    )
    qkv_local = [value.reshape(d_groups, share, -1) for value in qkv_sums]
    out_local = [value.reshape(heads, share, D) for value in out_sums]
    down_local = [value.reshape(d_groups, share, D) for value in down_sums]

    def in_order(items):
        return assemble([item[None] for item in items])

    qkv_slices = in_order(qkv_local)
    out_grad = jnp.transpose(
        in_order(out_local).reshape(QUERY_FEATURES // BLK, share, D), (1, 0, 2)
    ).astype(F32)
    down_grad = jnp.transpose(in_order(down_local).reshape(FF // BLK, share, D), (1, 0, 2)).astype(F32)

    def columns(value):
        return jnp.transpose(value, (2, 1, 0, 3)).reshape(share, d_groups, -1)

    qkv_grad = jnp.concatenate(
        [
            columns(qkv_slices[..., :query_slice]),
            columns(qkv_slices[..., query_slice : query_slice + key_slice]),
            columns(qkv_slices[..., query_slice + key_slice :]),
        ],
        axis=-1,
    ).astype(F32)
    geglu_slices = in_order([geglu_natural[turn] for turn in range(seq_count)])
    geglu_grad = jnp.transpose(geglu_slices, (3, 2, 1, 0, 4)).reshape(share, d_groups, 2 * FF).astype(F32)

    devices = lax.axis_size(ALL)
    capacity = first_moment.shape[0]
    stride = capacity + 1
    number = jnp.arange(block_owners.shape[0], dtype=jnp.int32)
    same = (block_owners[:, None] == block_owners[None, :]) & (number[None, :] < number[:, None])
    slots = block_owners * stride + jnp.sum(same.astype(jnp.int32), axis=1)

    gain_term = jnp.stack([gain_one, gain_two, gain_three, gain_four], axis=1)
    gain_share = D // devices
    gain_flat = gain_term.reshape(devices, gain_share * 4)
    gain_high = gain_flat.astype(BF16)
    gain_low = (gain_flat - gain_high.astype(F32)).astype(BF16)
    room = share * BLK
    gain_pair = jnp.concatenate([gain_high, gain_low], axis=1)
    extra = jnp.pad(gain_pair, ((0, 0), (0, room - gain_pair.shape[1]))).reshape(devices, share, BLK)

    ff_blocks = ff_slice // BLK
    out_base = d_groups * (QUERY_FEATURES + 2 * KEY_FEATURES) // BLK
    geglu_base = out_base + (QUERY_FEATURES // BLK) * (D // BLK)
    down_base = geglu_base + d_groups * 2 * FF // BLK
    if share % 8 == 0:
        pieces, layout = [], []
        query_blocks, key_blocks = query_slice // BLK, key_slice // BLK
        for turn in range(seq_count):
            qkv_columns = [(at, query_blocks, 0) for at in range(query_blocks)]
            for begin in (QUERY_FEATURES, QUERY_FEATURES + KEY_FEATURES):
                qkv_columns += [(begin // BLK + at, key_blocks, 0) for at in range(key_blocks)]
            pieces.append(qkv_local[turn])
            layout.append((turn, 0, (QUERY_FEATURES + 2 * KEY_FEATURES) // BLK, qkv_columns))
            pieces.append(out_local[turn])
            layout.append((turn, out_base, D // BLK, [(at, 0, heads) for at in range(D // BLK)]))
            for side in range(2):
                pieces.append(geglu_natural[turn, side])
                layout.append(
                    (
                        turn,
                        geglu_base,
                        2 * FF // BLK,
                        [(side * FF // BLK + at, ff_blocks, 0) for at in range(ff_blocks)],
                    )
                )
            pieces.append(down_local[turn])
            layout.append((turn, down_base, D // BLK, [(at, 0, d_groups) for at in range(D // BLK)]))
        outgoing = place_pieces(pieces, extra, slots, seq_index, layout, devices, stride)
    else:

        def to_pieces(gradient):
            count_of_rows, groups, col_count = gradient.shape
            shaped = gradient.astype(BF16).reshape(count_of_rows, groups, col_count // BLK, BLK)
            return jnp.transpose(shaped, (1, 2, 0, 3)).reshape(-1, count_of_rows, BLK)

        every = jnp.concatenate(
            [to_pieces(qkv_grad), to_pieces(out_grad), to_pieces(geglu_grad), to_pieces(down_grad)],
            axis=0,
        )
        outgoing = jnp.zeros((devices * stride, share, BLK), BF16).at[slots].set(every)
        outgoing = outgoing.at[jnp.arange(devices) * stride + capacity].set(extra)

    incoming = lax.all_to_all(outgoing, ALL, split_axis=0, concat_axis=0, tiled=True).reshape(
        devices, stride, share, BLK
    )
    gain_parts = incoming[:, capacity].reshape(devices, room)[:, : 2 * gain_share * 4].astype(F32)
    gain_sums = jnp.sum(gain_parts, axis=0)
    gains_grad = (gain_sums[: gain_share * 4] + gain_sums[gain_share * 4 :]).reshape(gain_share, 4)
    if share % 8 == 0:
        grads = incoming
    else:
        grads = jnp.transpose(incoming[:, :capacity], (1, 0, 2, 3)).reshape(capacity, BLK, BLK)
    first_new, second_new, weight_new = soap(
        grads, first_moment, second_moment, left_basis, right_basis, slot_weight
    )
    return (
        layer_out[None],
        row_rms[None],
        token_grad[None],
        qkv_grad,
        out_grad,
        geglu_grad,
        down_grad,
        gains_grad,
        first_new,
        second_new,
        weight_new,
    )


def solution(mesh):
    in_specs = (
        P("dp", "seq", None),
        P("dp", "seq", None),
        P(ALL, None, None),
        P(ALL, None, None),
        P(ALL, None, None),
        P(ALL, None, None),
        P(ALL, None),
        P("dp"),
        P("dp"),
        P(),
        P(ALL, None, None),
        P(ALL, None, None),
        P(ALL, None, None),
        P(ALL, None, None),
        P(ALL, None, None),
    )
    out_specs = (
        P("dp", "seq", None),
        P("dp", "seq"),
        P("dp", "seq", None),
        P(ALL, None, None),
        P(ALL, None, None),
        P(ALL, None, None),
        P(ALL, None, None),
        P(ALL, None),
        P(ALL, None, None),
        P(ALL, None, None),
        P(ALL, None, None),
    )
    return jax.shard_map(body, mesh=mesh, in_specs=in_specs, out_specs=out_specs, check_vma=False)
```

```python
import functools

import jax
import jax.numpy as jnp
from jax import lax
from jax.experimental import pallas as pl
from jax.experimental.pallas import tpu as pltpu
from jax.sharding import PartitionSpec as P


D = 2304
QUERY_HEADS = 8
HEAD_SIZE = 256
FF = 9216
BLK = 256
QUERY_FEATURES = 2048
KEY_FEATURES = 1024


EPSILON = 1e-06
SOFT_CAP = 50.0
NEGATIVE = -1e30
BETA_ONE = 0.9
BETA_TWO = 0.95
STEP_RATE = 0.05
TINY_ADD = 1e-08
CLIP_NORM = 1.0

F32 = jnp.float32
BF16 = jnp.bfloat16
ALL = ("seq", "dp")


def norm_forward(value_rows, gain):
    inverse = lax.rsqrt(jnp.mean(value_rows * value_rows, axis=-1, keepdims=True) + EPSILON)
    return (value_rows * inverse * gain, inverse)


def norm_backward(value_rows, inverse, gain, upstream):
    weighted = upstream * gain
    cubed = inverse * inverse * inverse
    grad_in = inverse * weighted - value_rows * cubed * jnp.mean(
        value_rows * weighted, axis=-1, keepdims=True
    )
    return (grad_in, jnp.sum(upstream * value_rows * inverse, axis=0))


def dot(left, right):
    return jnp.dot(left, right, preferred_element_type=F32)


def dot_nt(left, right):
    return lax.dot_general(left, right, (((1,), (1,)), ((), ())), preferred_element_type=F32)


def dot_tn(left, right):
    return lax.dot_general(left, right, (((0,), (0,)), ((), ())), preferred_element_type=F32)


def block_probs(query, keys, row_start, length, prefix):
    raw = dot_nt(query, keys)
    bent = jnp.tanh(raw * (HEAD_SIZE ** (-0.5) / SOFT_CAP))
    key_pos = lax.broadcasted_iota(jnp.int32, raw.shape, 1)
    query_pos = row_start + lax.broadcasted_iota(jnp.int32, raw.shape, 0)
    visible = (key_pos < length) & ((key_pos <= query_pos) | (key_pos < prefix))
    capped = jnp.where(visible, SOFT_CAP * bent, NEGATIVE)
    exponent = jnp.exp(capped - jnp.max(capped, axis=-1, keepdims=True))
    prob = exponent / jnp.sum(exponent, axis=-1, keepdims=True)
    return (prob, bent)


def attention_forward_kernel(heads, length_ref, prefix_ref, merged_ref, mixed_ref):
    length, prefix = length_ref[0], prefix_ref[0]
    key_col, value_col = heads * HEAD_SIZE, (heads + 1) * HEAD_SIZE
    tokens = merged_ref.shape[0]
    for head in range(heads):
        for start in range(0, tokens, BLK):
            rows, width = slice(start, start + BLK), start + BLK
            head_cols = slice(head * HEAD_SIZE, (head + 1) * HEAD_SIZE)
            keys = merged_ref[:width, key_col : key_col + HEAD_SIZE]
            values = merged_ref[:width, value_col : value_col + HEAD_SIZE]
            prob, _ = block_probs(merged_ref[rows, head_cols], keys, start, length, prefix)
            mixed_ref[rows, head_cols] = dot(prob.astype(BF16), values).astype(BF16)


def attention_backward_kernel(
    heads, length_ref, prefix_ref, merged_ref, upstream_ref, grad_ref, keys_acc, values_acc
):
    length, prefix = length_ref[0], prefix_ref[0]
    key_col, value_col = heads * HEAD_SIZE, (heads + 1) * HEAD_SIZE
    tokens = merged_ref.shape[0]
    keys_acc[...] = jnp.zeros_like(keys_acc)
    values_acc[...] = jnp.zeros_like(values_acc)
    for head in range(heads):
        for start in range(0, tokens, BLK):
            rows, width = slice(start, start + BLK), start + BLK
            head_cols = slice(head * HEAD_SIZE, (head + 1) * HEAD_SIZE)
            query = merged_ref[rows, head_cols]
            keys = merged_ref[:width, key_col : key_col + HEAD_SIZE]
            values = merged_ref[:width, value_col : value_col + HEAD_SIZE]
            upstream = upstream_ref[rows, head_cols]
            prob, bent = block_probs(query, keys, start, length, prefix)
            grad_prob = dot_nt(upstream, values)
            balance = jnp.sum(prob * grad_prob, axis=-1, keepdims=True)
            grad_raw = (
                prob * (grad_prob - balance) * (1.0 - bent * bent) * HEAD_SIZE ** (-0.5)
            ).astype(BF16)
            grad_ref[rows, head_cols] = dot(grad_raw, keys).astype(BF16)
            keys_acc[:width, :] += dot_tn(grad_raw, query)
            values_acc[:width, :] += dot_tn(prob.astype(BF16), upstream)
    grad_ref[:, key_col : key_col + HEAD_SIZE] = keys_acc[...].astype(BF16)
    grad_ref[:, value_col : value_col + HEAD_SIZE] = values_acc[...].astype(BF16)


SMEM_SPEC = pl.BlockSpec(memory_space=pltpu.SMEM)
VMEM_SPEC = pl.BlockSpec(memory_space=pltpu.VMEM)


def attention_forward(merged, length, prefix, heads):
    tokens = merged.shape[0]
    flops = 4 * heads * tokens * tokens * HEAD_SIZE
    return pl.pallas_call(
        functools.partial(attention_forward_kernel, heads),
        out_shape=jax.ShapeDtypeStruct((tokens, heads * HEAD_SIZE), BF16),
        in_specs=[SMEM_SPEC, SMEM_SPEC, VMEM_SPEC],
        out_specs=VMEM_SPEC,
        compiler_params=pltpu.CompilerParams(vmem_limit_bytes=40 << 20),
        cost_estimate=pl.CostEstimate(
            flops=flops, bytes_accessed=4 << 20, transcendentals=2 * heads * tokens * tokens
        ),
    )(length, prefix, merged)


def attention_backward(merged, upstream, length, prefix, heads):
    tokens = merged.shape[0]
    flops = 10 * heads * tokens * tokens * HEAD_SIZE
    return pl.pallas_call(
        functools.partial(attention_backward_kernel, heads),
        out_shape=jax.ShapeDtypeStruct(merged.shape, BF16),
        in_specs=[SMEM_SPEC, SMEM_SPEC, VMEM_SPEC, VMEM_SPEC],
        out_specs=VMEM_SPEC,
        scratch_shapes=[pltpu.VMEM((tokens, HEAD_SIZE), F32), pltpu.VMEM((tokens, HEAD_SIZE), F32)],
        compiler_params=pltpu.CompilerParams(vmem_limit_bytes=48 << 20),
        cost_estimate=pl.CostEstimate(
            flops=flops, bytes_accessed=6 << 20, transcendentals=2 * heads * tokens * tokens
        ),
    )(length, prefix, merged, upstream)


def place_kernel(layout, devices, stride, slots_ref, *refs):
    pieces, extra, out = refs[: len(layout)], refs[len(layout)], refs[len(layout) + 1]
    out[...] = jnp.zeros_like(out)

    @pl.loop(0, devices)
    def _(at):
        out[at * stride + stride - 1] = extra[at]

    seq_index = slots_ref[slots_ref.shape[0] - 1]
    for piece, (turn, base, per_row, columns) in zip(pieces, layout):
        source = jnp.bitwise_xor(seq_index, turn)

        @pl.loop(0, piece.shape[0])
        def _(a, piece=piece, base=base, per_row=per_row, columns=columns, source=source):
            for local, (fixed, factor, row_factor) in enumerate(columns):
                block = base + (a + source * row_factor) * per_row + fixed + source * factor
                out[slots_ref[block]] = piece[a, :, local * BLK : (local + 1) * BLK]


def place_pieces(pieces, extra, slots, seq_index, layout, devices, stride):
    share = extra.shape[1]
    table = jnp.concatenate([slots, seq_index[None]]).astype(jnp.int32)
    return pl.pallas_call(
        functools.partial(place_kernel, layout, devices, stride),
        out_shape=jax.ShapeDtypeStruct((devices * stride, share, BLK), BF16),
        in_specs=[SMEM_SPEC] + [VMEM_SPEC] * (len(pieces) + 1),
        out_specs=VMEM_SPEC,
        compiler_params=pltpu.CompilerParams(vmem_limit_bytes=48 << 20),
        cost_estimate=pl.CostEstimate(flops=0, bytes_accessed=12 << 20, transcendentals=0),
    )(table, *pieces, extra)


def soap_kernel(
    group, incoming, first, second, left, right, master, first_out, second_out, weight_out
):
    for at in range(group):
        if len(incoming.shape) == 4:
            grad = incoming[:, at].astype(F32).reshape(BLK, BLK)
        else:
            grad = incoming[at].astype(F32)
        size = jnp.sqrt(jnp.sum(grad * grad))
        scale = CLIP_NORM / jnp.maximum(size, CLIP_NORM)
        left_low = left[at].astype(BF16)
        right_low = right[at].astype(BF16)
        turned = dot_tn(left_low, grad.astype(BF16)).astype(BF16)
        rotated = dot(turned, right_low) * scale
        first_new = BETA_ONE * first[at] + (1.0 - BETA_ONE) * rotated
        second_new = BETA_TWO * second[at] + (1.0 - BETA_TWO) * rotated * rotated
        first_out[at] = first_new
        second_out[at] = second_new
        direction = (first_new / (jnp.sqrt(second_new) + TINY_ADD)).astype(BF16)
        back_left = dot(left_low, direction).astype(BF16)
        weight_out[at] = master[at] - STEP_RATE * dot_nt(back_left, right_low)


def soap(incoming, first, second, left, right, master):
    capacity = first.shape[0]
    group = 2 if capacity % 2 == 0 else 1
    spec = pl.BlockSpec((group, BLK, BLK), lambda at: (at, 0, 0))
    if incoming.ndim == 4:
        grad_spec = pl.BlockSpec(
            (incoming.shape[0], group) + incoming.shape[2:], lambda at: (0, at, 0, 0)
        )
    else:
        grad_spec = spec
    shape = jax.ShapeDtypeStruct(first.shape, F32)
    return pl.pallas_call(
        functools.partial(soap_kernel, group),
        grid=(capacity // group,),
        out_shape=(shape, shape, shape),
        in_specs=[grad_spec] + [spec] * 5,
        out_specs=(spec, spec, spec),
        compiler_params=pltpu.CompilerParams(vmem_limit_bytes=48 << 20),
        cost_estimate=pl.CostEstimate(
            flops=8 * capacity * BLK**3,
            bytes_accessed=34 * capacity * BLK * BLK,
            transcendentals=2 * capacity * BLK * BLK,
        ),
    )(incoming, first, second, left, right, master)


def body(
    tokens,
    cotangent,
    qkv_weight,
    out_weight,
    geglu_weight,
    down_weight,
    norm_gains,
    seq_lengths,
    prefix_lengths,
    block_owners,
    first_moment,
    second_moment,
    left_basis,
    right_basis,
    slot_weight,
):
    inputs = tokens[0].astype(F32)
    upstream = cotangent[0].astype(F32)
    rows = inputs.shape[0]
    seq_count = lax.axis_size("seq")
    dp_count = lax.axis_size("dp")
    seq_index = lax.axis_index("seq")
    share = qkv_weight.shape[0]
    heads = QUERY_HEADS // seq_count
    query_slice = heads * HEAD_SIZE
    key_slice = KEY_FEATURES // seq_count
    ff_slice = FF // seq_count
    d_groups = D // BLK
    half = ff_slice // 2
    parts = (slice(0, D // 3), slice(D // 3, D))

    def swap(value, turn):
        return lax.ppermute(value, "seq", [(at, at ^ turn) for at in range(seq_count)])

    def double_gather(value):
        for axis, size in (("dp", dp_count), ("seq", seq_count)):
            step = 1
            while step < size:
                other = lax.ppermute(value, axis, [(at, at ^ step) for at in range(size)])
                upper = (lax.axis_index(axis) & step) != 0
                value = jnp.concatenate(
                    [jnp.where(upper, other, value), jnp.where(upper, value, other)], axis=0
                )
                step *= 2
        return value

    def owner_of(turn):
        return jnp.bitwise_xor(seq_index, turn)

    def pick(value, index, size, axis):
        return lax.dynamic_slice_in_dim(value, index * size, size, axis)

    def assemble(items):
        size = items[0].shape[0]
        buffer = jnp.zeros((size * seq_count,) + items[0].shape[1:], items[0].dtype)
        for turn, item in enumerate(items):
            start = (owner_of(turn) * size,) + (0,) * (item.ndim - 1)
            buffer = lax.dynamic_update_slice(buffer, item, start)
        return buffer

    def gather_rows(value):
        received = {turn: swap(value, turn) for turn in range(seq_count - 1, 0, -1)}
        return assemble([value] + [received[turn] for turn in range(1, seq_count)])

    def scatter_rows(part_of):
        received = []
        for turn in range(seq_count - 1, 0, -1):
            received.append(swap(part_of(owner_of(turn)).astype(BF16), turn))
        result = part_of(seq_index)
        for value in received:
            result = result + value.astype(F32)
        return result

    def spread(piece_for):
        received = [piece_for(seq_index)]
        for turn in range(1, seq_count):
            received.append(swap(piece_for(owner_of(turn)), turn))
        operand = assemble(received)
        return lax.all_gather(operand, "dp", axis=0, tiled=True)

    def collect(gradient):
        summed = lax.psum_scatter(gradient, "dp", scatter_dimension=0, tiled=True)
        size = summed.shape[0] // seq_count
        result = [pick(summed, seq_index, size, 0)]
        for turn in range(1, seq_count):
            result.append(swap(pick(summed, owner_of(turn), size, 0), turn))
        return result

    def after(values, others):
        return list(lax.optimization_barrier(tuple(values) + tuple(others)))[: len(values)]

    def row_order(groups):
        at = jnp.arange(groups * BLK, dtype=jnp.int32)
        inner = at % share
        group = (at // share) % groups
        device = at // (share * groups)
        natural = share * (dp_count * (device % seq_count) + device // seq_count) + inner
        return group * BLK + natural

    def order_matrix(groups):
        return (jnp.arange(groups * BLK, dtype=jnp.int32)[:, None] == row_order(groups)[None, :]).astype(BF16)

    wide_order = order_matrix(d_groups)
    head_order = order_matrix(heads)

    def local_rows(weight):
        return jnp.transpose(weight.astype(BF16), (1, 0, 2))

    qkv_low = local_rows(qkv_weight).reshape(d_groups * share, -1)
    out_low = local_rows(out_weight)
    down_low = local_rows(down_weight)
    gain_full = double_gather(norm_gains.astype(BF16).reshape(1, -1)).reshape(D, 4)

    def qkv_piece(target):
        return jnp.concatenate(
            [
                pick(qkv_low[:, :QUERY_FEATURES], target, query_slice, 1),
                pick(qkv_low[:, QUERY_FEATURES : QUERY_FEATURES + KEY_FEATURES], target, key_slice, 1),
                pick(qkv_low[:, QUERY_FEATURES + KEY_FEATURES :], target, key_slice, 1),
            ],
            axis=1,
        )

    def out_piece(target):
        return pick(out_low, target, heads, 0).reshape(heads * share, D)

    def down_piece(part):
        return lambda target: pick(down_low[..., part], target, d_groups, 0).reshape(
            d_groups * share, -1
        )

    qkv_slice_full = spread(qkv_piece)
    out_slice_full = spread(out_piece)

    geglu_rows = jnp.transpose(
        geglu_weight.astype(BF16).reshape(share, d_groups, 2 * seq_count, ff_slice), (2, 1, 0, 3)
    ).reshape(2 * seq_count * d_groups * share, ff_slice)
    geglu_turned = dot(geglu_rows, wide_order).astype(BF16).reshape(
        2 * seq_count, d_groups * share, ff_slice
    )

    def geglu_piece(part):
        cols = slice(part * half, (part + 1) * half)

        def piece(target):
            return jnp.concatenate(
                [
                    lax.dynamic_index_in_dim(geglu_turned, target, 0, False)[:, cols],
                    lax.dynamic_index_in_dim(geglu_turned, target + seq_count, 0, False)[:, cols],
                ],
                axis=1,
            )

        return piece

    geglu_zero = spread(geglu_piece(0))
    geglu_one = spread(geglu_piece(1))
    geglu_parts = (geglu_zero, geglu_one)
    down_late = spread(down_piece(parts[1]))
    down_early = spread(down_piece(parts[0]))

    gains = gain_full.astype(F32)
    normed, inverse_one = norm_forward(inputs, gains[:, 0])
    normed_turned = dot(normed.astype(BF16), wide_order).astype(BF16)
    normed_all = gather_rows(normed_turned)
    merged = dot(normed_all, qkv_slice_full).astype(BF16)
    mixed = attention_forward(merged, seq_lengths, prefix_lengths, heads)
    mixed_turned = dot(mixed, head_order).astype(BF16)
    attended = scatter_rows(lambda owner: dot(pick(mixed_turned, owner, rows, 0), out_slice_full))
    attn_normed, inverse_two = norm_forward(attended, gains[:, 1])
    hidden = inputs + attn_normed
    ffn_normed, inverse_three = norm_forward(hidden, gains[:, 2])
    ffn_turned = dot(ffn_normed.astype(BF16), wide_order).astype(BF16)
    ffn_all = gather_rows(ffn_turned)

    gates, uppers, products = [], [], []
    for part in range(2):
        gate_up = dot(ffn_all, geglu_parts[part])
        gate, upper = gate_up[:, :half], gate_up[:, half:]
        gates.append(gate)
        uppers.append(upper)
        products.append((jax.nn.gelu(gate, approximate=True) * upper).astype(BF16))

    product = jnp.concatenate(products, axis=1)

    def branch_columns(weight):
        def part_of(owner):
            return dot(pick(product, owner, rows, 0), weight)

        return scatter_rows(part_of)

    branch_late = branch_columns(down_late)
    branch = jnp.concatenate([branch_columns(down_early), branch_late], axis=1)
    branch_normed, inverse_four = norm_forward(branch, gains[:, 3])
    query_pos = seq_index * rows + jnp.arange(rows, dtype=jnp.int32)
    live_rows = (query_pos < seq_lengths[0]).astype(F32)[:, None]
    layer_out = ((hidden + branch_normed) * live_rows).astype(BF16)
    row_rms = jnp.sqrt(jnp.mean(inputs * inputs, axis=-1) + EPSILON)

    upstream = upstream * live_rows
    grad_branch, gain_four = norm_backward(branch, inverse_four, gains[:, 3], upstream)
    branch_low = grad_branch.astype(BF16)
    branch_alls = [gather_rows(branch_low[:, part]) for part in parts]
    down_terms = []
    for value in branch_alls:
        down_terms.append(dot_tn(product, value).astype(BF16))
    down_sums = [collect(term) for term in down_terms]
    branch_alls = after(branch_alls, down_terms)
    gate_up_grads = []
    geglu_terms = []
    for part in range(2):
        ff_rows = slice(part * half, (part + 1) * half)
        grad_product = dot_nt(branch_alls[0], down_early[ff_rows]) + dot_nt(
            branch_alls[1], down_late[ff_rows]
        )
        activated, gelu_pull = jax.vjp(lambda value: jax.nn.gelu(value, approximate=True), gates[part])
        grad_gate = gelu_pull(grad_product * uppers[part])[0]
        grad_upper = grad_product * activated
        gate_up_grad = jnp.concatenate([grad_gate, grad_upper], axis=1).astype(BF16)
        geglu_terms.append(dot_tn(ffn_all, gate_up_grad).astype(BF16))
        if part == 0:
            branch_alls = after(branch_alls, [geglu_terms[0]])
        gate_up_grads.append(gate_up_grad)
    geglu_sums = [collect(term) for term in geglu_terms]
    ffn_total = dot_nt(gate_up_grads[0], geglu_zero) + dot_nt(gate_up_grads[1], geglu_one)

    def ffn_part(owner):
        return pick(ffn_total, owner, rows, 0)

    grad_ffn = dot_nt(scatter_rows(ffn_part).astype(BF16), wide_order)
    grad_hidden_norm, gain_three = norm_backward(hidden, inverse_three, gains[:, 2], grad_ffn)
    grad_hidden = upstream + grad_hidden_norm
    grad_attended, gain_two = norm_backward(attended, inverse_two, gains[:, 1], grad_hidden)
    attended_all = gather_rows(grad_attended.astype(BF16))
    (attended_all,) = after([attended_all], [geglu_terms[1]])
    grad_mixed_turned = dot_nt(attended_all, out_slice_full).astype(BF16)
    grad_mixed = dot_nt(grad_mixed_turned, head_order).astype(BF16)
    out_term = dot_tn(mixed_turned, attended_all).astype(BF16)
    out_sums = collect(out_term)
    (grad_mixed,) = after([grad_mixed], [out_term])
    grad_merged = attention_backward(merged, grad_mixed, seq_lengths, prefix_lengths, heads)
    qkv_sums = collect(dot_tn(normed_all, grad_merged).astype(BF16))
    grad_normed = dot_nt(
        scatter_rows(lambda owner: dot_nt(pick(grad_merged, owner, rows, 0), qkv_slice_full)).astype(BF16),
        wide_order,
    )
    grad_input_norm, gain_one = norm_backward(inputs, inverse_one, gains[:, 0], grad_normed)
    token_grad = grad_hidden + grad_input_norm

    turned = jnp.concatenate(
        [
            jnp.concatenate(
                [geglu_sums[0][turn][:, side * half : (side + 1) * half],
                 geglu_sums[1][turn][:, side * half : (side + 1) * half]],
                axis=1,
            )
            for turn in range(seq_count)
            for side in range(2)
        ],
        axis=0,
    )
    geglu_natural = dot_nt(turned, wide_order).astype(BF16)
    geglu_natural = geglu_natural.reshape(
        seq_count, 2, d_groups, share, ff_slice
    )
    qkv_local = [value.reshape(d_groups, share, -1) for value in qkv_sums]
    out_local = [value.reshape(heads, share, D) for value in out_sums]
    down_local = [
        jnp.concatenate([early, late], axis=1).reshape(d_groups, share, D)
        for early, late in zip(*down_sums)
    ]

    def in_order(items):
        return assemble([item[None] for item in items])

    qkv_slices = in_order(qkv_local)
    out_grad = jnp.transpose(
        in_order(out_local).reshape(QUERY_FEATURES // BLK, share, D), (1, 0, 2)
    ).astype(F32)
    down_grad = jnp.transpose(in_order(down_local).reshape(FF // BLK, share, D), (1, 0, 2)).astype(F32)

    def columns(value):
        return jnp.transpose(value, (2, 1, 0, 3)).reshape(share, d_groups, -1)

    qkv_grad = jnp.concatenate(
        [
            columns(qkv_slices[..., :query_slice]),
            columns(qkv_slices[..., query_slice : query_slice + key_slice]),
            columns(qkv_slices[..., query_slice + key_slice :]),
        ],
        axis=-1,
    ).astype(F32)
    geglu_slices = in_order([geglu_natural[turn] for turn in range(seq_count)])
    geglu_grad = jnp.transpose(geglu_slices, (3, 2, 1, 0, 4)).reshape(share, d_groups, 2 * FF).astype(F32)

    devices = lax.axis_size(ALL)
    capacity = first_moment.shape[0]
    stride = capacity + 1
    number = jnp.arange(block_owners.shape[0], dtype=jnp.int32)
    same = (block_owners[:, None] == block_owners[None, :]) & (number[None, :] < number[:, None])
    slots = block_owners * stride + jnp.sum(same.astype(jnp.int32), axis=1)

    gain_term = jnp.stack([gain_one, gain_two, gain_three, gain_four], axis=1)
    gain_share = D // devices
    gain_flat = gain_term.reshape(devices, gain_share * 4)
    gain_high = gain_flat.astype(BF16)
    gain_low = (gain_flat - gain_high.astype(F32)).astype(BF16)
    room = share * BLK
    gain_pair = jnp.concatenate([gain_high, gain_low], axis=1)
    extra = jnp.pad(gain_pair, ((0, 0), (0, room - gain_pair.shape[1]))).reshape(devices, share, BLK)

    ff_blocks = ff_slice // BLK
    out_base = d_groups * (QUERY_FEATURES + 2 * KEY_FEATURES) // BLK
    geglu_base = out_base + (QUERY_FEATURES // BLK) * (D // BLK)
    down_base = geglu_base + d_groups * 2 * FF // BLK
    if share % 8 == 0:
        pieces, layout = [], []
        query_blocks, key_blocks = query_slice // BLK, key_slice // BLK
        for turn in range(seq_count):
            qkv_columns = [(at, query_blocks, 0) for at in range(query_blocks)]
            for begin in (QUERY_FEATURES, QUERY_FEATURES + KEY_FEATURES):
                qkv_columns += [(begin // BLK + at, key_blocks, 0) for at in range(key_blocks)]
            pieces.append(qkv_local[turn])
            layout.append((turn, 0, (QUERY_FEATURES + 2 * KEY_FEATURES) // BLK, qkv_columns))
            pieces.append(out_local[turn])
            layout.append((turn, out_base, D // BLK, [(at, 0, heads) for at in range(D // BLK)]))
            for side in range(2):
                pieces.append(geglu_natural[turn, side])
                layout.append(
                    (
                        turn,
                        geglu_base,
                        2 * FF // BLK,
                        [(side * FF // BLK + at, ff_blocks, 0) for at in range(ff_blocks)],
                    )
                )
            pieces.append(down_local[turn])
            layout.append((turn, down_base, D // BLK, [(at, 0, d_groups) for at in range(D // BLK)]))
        outgoing = place_pieces(pieces, extra, slots, seq_index, layout, devices, stride)
    else:

        def to_pieces(gradient):
            count_of_rows, groups, col_count = gradient.shape
            shaped = gradient.astype(BF16).reshape(count_of_rows, groups, col_count // BLK, BLK)
            return jnp.transpose(shaped, (1, 2, 0, 3)).reshape(-1, count_of_rows, BLK)

        every = jnp.concatenate(
            [to_pieces(qkv_grad), to_pieces(out_grad), to_pieces(geglu_grad), to_pieces(down_grad)],
            axis=0,
        )
        outgoing = jnp.zeros((devices * stride, share, BLK), BF16).at[slots].set(every)
        outgoing = outgoing.at[jnp.arange(devices) * stride + capacity].set(extra)

    incoming = lax.all_to_all(outgoing, ALL, split_axis=0, concat_axis=0, tiled=True).reshape(
        devices, stride, share, BLK
    )
    gain_parts = incoming[:, capacity].reshape(devices, room)[:, : 2 * gain_share * 4].astype(F32)
    gain_sums = jnp.sum(gain_parts, axis=0)
    gains_grad = (gain_sums[: gain_share * 4] + gain_sums[gain_share * 4 :]).reshape(gain_share, 4)
    if share % 8 == 0:
        grads = incoming
    else:
        grads = jnp.transpose(incoming[:, :capacity], (1, 0, 2, 3)).reshape(capacity, BLK, BLK)
    first_new, second_new, weight_new = soap(
        grads, first_moment, second_moment, left_basis, right_basis, slot_weight
    )
    return (
        layer_out[None],
        row_rms[None],
        token_grad[None],
        qkv_grad,
        out_grad,
        geglu_grad,
        down_grad,
        gains_grad,
        first_new,
        second_new,
        weight_new,
    )


def solution(mesh):
    in_specs = (
        P("dp", "seq", None),
        P("dp", "seq", None),
        P(ALL, None, None),
        P(ALL, None, None),
        P(ALL, None, None),
        P(ALL, None, None),
        P(ALL, None),
        P("dp"),
        P("dp"),
        P(),
        P(ALL, None, None),
        P(ALL, None, None),
        P(ALL, None, None),
        P(ALL, None, None),
        P(ALL, None, None),
    )
    out_specs = (
        P("dp", "seq", None),
        P("dp", "seq"),
        P("dp", "seq", None),
        P(ALL, None, None),
        P(ALL, None, None),
        P(ALL, None, None),
        P(ALL, None, None),
        P(ALL, None),
        P(ALL, None, None),
        P(ALL, None, None),
        P(ALL, None, None),
    )

    return jax.shard_map(body, mesh=mesh, in_specs=in_specs, out_specs=out_specs, check_vma=False)
```

```python
import functools

import jax
import jax.numpy as jnp
from jax import lax
from jax.experimental import pallas as pl
from jax.experimental.pallas import tpu as pltpu
from jax.sharding import PartitionSpec as P


D = 2304
QUERY_HEADS = 8
HEAD_SIZE = 256
FF = 9216
BLK = 256
QUERY_FEATURES = 2048
KEY_FEATURES = 1024


EPSILON = 1e-06
SOFT_CAP = 50.0
NEGATIVE = -1e30
BETA_ONE = 0.9
BETA_TWO = 0.95
STEP_RATE = 0.05
TINY_ADD = 1e-08
CLIP_NORM = 1.0

F32 = jnp.float32
BF16 = jnp.bfloat16
ALL = ("seq", "dp")


def norm_forward(value_rows, gain):
    inverse = lax.rsqrt(jnp.mean(value_rows * value_rows, axis=-1, keepdims=True) + EPSILON)
    return (value_rows * inverse * gain, inverse)


def norm_backward(value_rows, inverse, gain, upstream):
    weighted = upstream * gain
    cubed = inverse * inverse * inverse
    grad_in = inverse * weighted - value_rows * cubed * jnp.mean(
        value_rows * weighted, axis=-1, keepdims=True
    )
    return (grad_in, jnp.sum(upstream * value_rows * inverse, axis=0))


def dot(left, right):
    return jnp.dot(left, right, preferred_element_type=F32)


def dot_nt(left, right):
    return lax.dot_general(left, right, (((1,), (1,)), ((), ())), preferred_element_type=F32)


def dot_tn(left, right):
    return lax.dot_general(left, right, (((0,), (0,)), ((), ())), preferred_element_type=F32)


def block_probs(query, keys, row_start, length, prefix):
    raw = dot_nt(query, keys)
    bent = jnp.tanh(raw * (HEAD_SIZE ** (-0.5) / SOFT_CAP))
    key_pos = lax.broadcasted_iota(jnp.int32, raw.shape, 1)
    query_pos = row_start + lax.broadcasted_iota(jnp.int32, raw.shape, 0)
    visible = (key_pos < length) & ((key_pos <= query_pos) | (key_pos < prefix))
    capped = jnp.where(visible, SOFT_CAP * bent, NEGATIVE)
    exponent = jnp.exp(capped - jnp.max(capped, axis=-1, keepdims=True))
    prob = exponent / jnp.sum(exponent, axis=-1, keepdims=True)
    return (prob, bent)


def attention_forward_kernel(heads, length_ref, prefix_ref, merged_ref, mixed_ref):
    length, prefix = length_ref[0], prefix_ref[0]
    key_col, value_col = heads * HEAD_SIZE, (heads + 1) * HEAD_SIZE
    tokens = merged_ref.shape[0]
    for head in range(heads):
        for start in range(0, tokens, BLK):
            rows, width = slice(start, start + BLK), start + BLK
            head_cols = slice(head * HEAD_SIZE, (head + 1) * HEAD_SIZE)
            keys = merged_ref[:width, key_col : key_col + HEAD_SIZE]
            values = merged_ref[:width, value_col : value_col + HEAD_SIZE]
            prob, _ = block_probs(merged_ref[rows, head_cols], keys, start, length, prefix)
            mixed_ref[rows, head_cols] = dot(prob.astype(BF16), values).astype(BF16)


def attention_backward_kernel(
    heads, length_ref, prefix_ref, merged_ref, upstream_ref, grad_ref, keys_acc, values_acc
):
    length, prefix = length_ref[0], prefix_ref[0]
    key_col, value_col = heads * HEAD_SIZE, (heads + 1) * HEAD_SIZE
    tokens = merged_ref.shape[0]
    keys_acc[...] = jnp.zeros_like(keys_acc)
    values_acc[...] = jnp.zeros_like(values_acc)
    for head in range(heads):
        for start in range(0, tokens, BLK):
            rows, width = slice(start, start + BLK), start + BLK
            head_cols = slice(head * HEAD_SIZE, (head + 1) * HEAD_SIZE)
            query = merged_ref[rows, head_cols]
            keys = merged_ref[:width, key_col : key_col + HEAD_SIZE]
            values = merged_ref[:width, value_col : value_col + HEAD_SIZE]
            upstream = upstream_ref[rows, head_cols]
            prob, bent = block_probs(query, keys, start, length, prefix)
            grad_prob = dot_nt(upstream, values)
            balance = jnp.sum(prob * grad_prob, axis=-1, keepdims=True)
            grad_raw = (
                prob * (grad_prob - balance) * (1.0 - bent * bent) * HEAD_SIZE ** (-0.5)
            ).astype(BF16)
            grad_ref[rows, head_cols] = dot(grad_raw, keys).astype(BF16)
            keys_acc[:width, :] += dot_tn(grad_raw, query)
            values_acc[:width, :] += dot_tn(prob.astype(BF16), upstream)
    grad_ref[:, key_col : key_col + HEAD_SIZE] = keys_acc[...].astype(BF16)
    grad_ref[:, value_col : value_col + HEAD_SIZE] = values_acc[...].astype(BF16)


SMEM_SPEC = pl.BlockSpec(memory_space=pltpu.SMEM)
VMEM_SPEC = pl.BlockSpec(memory_space=pltpu.VMEM)


def attention_forward(merged, length, prefix, heads):
    tokens = merged.shape[0]
    flops = 4 * heads * tokens * tokens * HEAD_SIZE
    return pl.pallas_call(
        functools.partial(attention_forward_kernel, heads),
        out_shape=jax.ShapeDtypeStruct((tokens, heads * HEAD_SIZE), BF16),
        in_specs=[SMEM_SPEC, SMEM_SPEC, VMEM_SPEC],
        out_specs=VMEM_SPEC,
        compiler_params=pltpu.CompilerParams(vmem_limit_bytes=40 << 20),
        cost_estimate=pl.CostEstimate(
            flops=flops, bytes_accessed=4 << 20, transcendentals=2 * heads * tokens * tokens
        ),
    )(length, prefix, merged)


def attention_backward(merged, upstream, length, prefix, heads):
    tokens = merged.shape[0]
    flops = 10 * heads * tokens * tokens * HEAD_SIZE
    return pl.pallas_call(
        functools.partial(attention_backward_kernel, heads),
        out_shape=jax.ShapeDtypeStruct(merged.shape, BF16),
        in_specs=[SMEM_SPEC, SMEM_SPEC, VMEM_SPEC, VMEM_SPEC],
        out_specs=VMEM_SPEC,
        scratch_shapes=[pltpu.VMEM((tokens, HEAD_SIZE), F32), pltpu.VMEM((tokens, HEAD_SIZE), F32)],
        compiler_params=pltpu.CompilerParams(vmem_limit_bytes=48 << 20),
        cost_estimate=pl.CostEstimate(
            flops=flops, bytes_accessed=6 << 20, transcendentals=2 * heads * tokens * tokens
        ),
    )(length, prefix, merged, upstream)


def place_kernel(layout, devices, sizes, slots_ref, *refs):
    count = len(refs) - 4
    pieces, extra, out_one, out_two, flat = refs[:count], refs[count], *refs[count + 1 :]
    flat[...] = jnp.zeros_like(flat)
    split = devices * sizes[0]

    @pl.loop(0, devices)
    def _(at):
        flat[split + (at + 1) * sizes[1] - 1] = extra[at]

    seq_index = slots_ref[slots_ref.shape[0] - 1]
    for index, turn, base, per_row, columns in layout:
        piece = pieces[index]
        source = jnp.bitwise_xor(seq_index, turn)

        @pl.loop(0, piece.shape[0])
        def _(a, piece=piece, base=base, per_row=per_row, columns=columns, source=source):
            for local, fixed, factor, row_factor in columns:
                block = base + (a + source * row_factor) * per_row + fixed + source * factor
                flat[slots_ref[block]] = piece[a, :, local * BLK : (local + 1) * BLK]

    out_one[...] = flat[:split]
    out_two[...] = flat[split:]


def place_pieces(pieces, extra, slots, seq_index, layout, devices, sizes):
    share = extra.shape[1]
    table = jnp.concatenate([slots, seq_index[None]]).astype(jnp.int32)
    return pl.pallas_call(
        functools.partial(place_kernel, layout, devices, sizes),
        out_shape=tuple(jax.ShapeDtypeStruct((devices * size, share, BLK), BF16) for size in sizes),
        in_specs=[SMEM_SPEC] + [VMEM_SPEC] * (len(pieces) + 1),
        out_specs=(VMEM_SPEC, VMEM_SPEC),
        scratch_shapes=[pltpu.VMEM((devices * sum(sizes), share, BLK), BF16)],
        compiler_params=pltpu.CompilerParams(vmem_limit_bytes=48 << 20),
        cost_estimate=pl.CostEstimate(flops=0, bytes_accessed=12 << 20, transcendentals=0),
    )(table, *pieces, extra)


def soap_kernel(group, incoming, first, second, left, right, master, *outs):
    first_out, second_out, weight_out = outs[-3:]
    for at in range(group):
        if len(incoming.shape) == 4:
            grad = incoming[:, at].astype(F32).reshape(BLK, BLK)
        else:
            grad = incoming[at].astype(F32)
        size = jnp.sqrt(jnp.sum(grad * grad))
        scale = CLIP_NORM / jnp.maximum(size, CLIP_NORM)
        left_low = left[at].astype(BF16)
        right_low = right[at].astype(BF16)
        turned = dot_tn(left_low, grad.astype(BF16)).astype(BF16)
        rotated = dot(turned, right_low) * scale
        first_new = BETA_ONE * first[at] + (1.0 - BETA_ONE) * rotated
        second_new = BETA_TWO * second[at] + (1.0 - BETA_TWO) * rotated * rotated
        first_out[at] = first_new
        second_out[at] = second_new
        direction = (first_new / (jnp.sqrt(second_new) + TINY_ADD)).astype(BF16)
        back_left = dot(left_low, direction).astype(BF16)
        weight_out[at] = master[at] - STEP_RATE * dot_nt(back_left, right_low)


def soap(incoming, state, begin, count, earlier):
    capacity = state[0].shape[0]
    group = 2 if begin % 2 == 0 and count % 2 == 0 else 1
    spec = pl.BlockSpec((group, BLK, BLK), lambda at: (at + begin // group, 0, 0))
    if incoming.ndim == 4:
        grad_spec = pl.BlockSpec(
            (incoming.shape[0], group) + incoming.shape[2:], lambda at: (0, at, 0, 0)
        )
    else:
        grad_spec = pl.BlockSpec((group, BLK, BLK), lambda at: (at, 0, 0))
    shape = jax.ShapeDtypeStruct((capacity, BLK, BLK), F32)
    return pl.pallas_call(
        functools.partial(soap_kernel, group),
        grid=(count // group,),
        out_shape=(shape, shape, shape),
        in_specs=[grad_spec] + [spec] * 5 + [pl.BlockSpec(memory_space=pl.ANY)] * len(earlier),
        out_specs=(spec, spec, spec),
        input_output_aliases={6 + at: at for at in range(len(earlier))},
        compiler_params=pltpu.CompilerParams(vmem_limit_bytes=48 << 20),
        cost_estimate=pl.CostEstimate(
            flops=8 * count * BLK**3,
            bytes_accessed=34 * count * BLK * BLK,
            transcendentals=2 * count * BLK * BLK,
        ),
    )(incoming, *state, *earlier)


def body(
    tokens,
    cotangent,
    qkv_weight,
    out_weight,
    geglu_weight,
    down_weight,
    norm_gains,
    seq_lengths,
    prefix_lengths,
    block_owners,
    first_moment,
    second_moment,
    left_basis,
    right_basis,
    slot_weight,
):
    inputs = tokens[0].astype(F32)
    upstream = cotangent[0].astype(F32)
    rows = inputs.shape[0]
    seq_count = lax.axis_size("seq")
    dp_count = lax.axis_size("dp")
    seq_index = lax.axis_index("seq")
    share = qkv_weight.shape[0]
    heads = QUERY_HEADS // seq_count
    query_slice = heads * HEAD_SIZE
    key_slice = KEY_FEATURES // seq_count
    ff_slice = FF // seq_count
    d_groups = D // BLK
    cut = D * 5 // 18
    parts = (slice(0, cut), slice(cut, D))
    qkv_slice = query_slice + 2 * key_slice

    def swap(value, turn):
        return lax.ppermute(value, "seq", [(at, at ^ turn) for at in range(seq_count)])

    def double_gather(value):
        for axis, size in (("dp", dp_count), ("seq", seq_count)):
            step = 1
            while step < size:
                other = lax.ppermute(value, axis, [(at, at ^ step) for at in range(size)])
                upper = (lax.axis_index(axis) & step) != 0
                value = jnp.concatenate(
                    [jnp.where(upper, other, value), jnp.where(upper, value, other)], axis=0
                )
                step *= 2
        return value

    def owner_of(turn):
        return jnp.bitwise_xor(seq_index, turn)

    def pick(value, index, size, axis):
        return lax.dynamic_slice_in_dim(value, index * size, size, axis)

    def assemble(items):
        size = items[0].shape[0]
        buffer = jnp.zeros((size * seq_count,) + items[0].shape[1:], items[0].dtype)
        for turn, item in enumerate(items):
            start = (owner_of(turn) * size,) + (0,) * (item.ndim - 1)
            buffer = lax.dynamic_update_slice(buffer, item, start)
        return buffer

    def gather_rows(value):
        received = {turn: swap(value, turn) for turn in range(seq_count - 1, 0, -1)}
        return assemble([value] + [received[turn] for turn in range(1, seq_count)])

    def scatter_rows(part_of):
        received = []
        for turn in range(seq_count - 1, 0, -1):
            received.append(swap(part_of(owner_of(turn)).astype(BF16), turn))
        result = part_of(seq_index)
        for value in received:
            result = result + value.astype(F32)
        return result

    def spread(piece_for):
        received = [piece_for(seq_index)]
        for turn in range(1, seq_count):
            received.append(swap(piece_for(owner_of(turn)), turn))
        operand = assemble(received)
        return lax.all_gather(operand, "dp", axis=0, tiled=True)

    def collect(gradient):
        summed = lax.psum_scatter(gradient, "dp", scatter_dimension=0, tiled=True)
        size = summed.shape[0] // seq_count
        result = [pick(summed, seq_index, size, 0)]
        for turn in range(1, seq_count):
            result.append(swap(pick(summed, owner_of(turn), size, 0), turn))
        return result

    def after(values, others):
        return list(lax.optimization_barrier(tuple(values) + tuple(others)))[: len(values)]

    def row_order(groups):
        at = jnp.arange(groups * BLK, dtype=jnp.int32)
        inner = at % share
        group = (at // share) % groups
        device = at // (share * groups)
        natural = share * (dp_count * (device % seq_count) + device // seq_count) + inner
        return group * BLK + natural

    def order_matrix(groups):
        return (jnp.arange(groups * BLK, dtype=jnp.int32)[:, None] == row_order(groups)[None, :]).astype(BF16)

    wide_order = order_matrix(d_groups)
    head_order = order_matrix(heads)

    def local_rows(weight):
        return jnp.transpose(weight.astype(BF16), (1, 0, 2))

    qkv_low = local_rows(qkv_weight).reshape(d_groups * share, -1)
    out_low = local_rows(out_weight)
    down_low = local_rows(down_weight)
    gain_full = double_gather(norm_gains.astype(BF16).reshape(1, -1)).reshape(D, 4)

    def out_piece(target):
        piece = pick(out_low, target, heads, 0).reshape(heads, share, d_groups, BLK)
        return jnp.transpose(piece, (2, 1, 0, 3)).reshape(d_groups * share, query_slice)

    def qkv_piece(target):
        return jnp.concatenate(
            [
                pick(qkv_low[:, :QUERY_FEATURES], target, query_slice, 1),
                pick(qkv_low[:, QUERY_FEATURES : QUERY_FEATURES + KEY_FEATURES], target, key_slice, 1),
                pick(qkv_low[:, QUERY_FEATURES + KEY_FEATURES :], target, key_slice, 1),
                out_piece(target),
            ],
            axis=1,
        )

    def down_piece(part):
        return lambda target: pick(down_low[..., part], target, d_groups, 0).reshape(
            d_groups * share, -1
        )

    heads_full = spread(qkv_piece)
    qkv_slice_full = heads_full[:, :qkv_slice]
    out_slice_full = jnp.transpose(
        heads_full[:, qkv_slice:].reshape(-1, d_groups, share, heads, BLK), (0, 3, 2, 1, 4)
    ).reshape(query_slice, D)

    geglu_rows = jnp.transpose(
        geglu_weight.astype(BF16).reshape(share, d_groups, 2 * seq_count, ff_slice), (2, 1, 0, 3)
    ).reshape(2 * seq_count * d_groups * share, ff_slice)
    geglu_turned = dot(geglu_rows, wide_order).astype(BF16).reshape(
        2 * seq_count, d_groups * share, ff_slice
    )

    def geglu_piece(target):
        return jnp.concatenate(
            [
                lax.dynamic_index_in_dim(geglu_turned, target, 0, False),
                lax.dynamic_index_in_dim(geglu_turned, target + seq_count, 0, False),
            ],
            axis=1,
        )

    geglu_full = spread(geglu_piece)
    down_late = spread(down_piece(parts[1]))
    down_early = spread(down_piece(parts[0]))

    gains = gain_full.astype(F32)
    normed, inverse_one = norm_forward(inputs, gains[:, 0])
    normed_turned = dot(normed.astype(BF16), wide_order).astype(BF16)
    normed_all = gather_rows(normed_turned)
    merged = dot(normed_all, qkv_slice_full).astype(BF16)
    mixed = attention_forward(merged, seq_lengths, prefix_lengths, heads)
    mixed_turned = dot(mixed, head_order).astype(BF16)
    attended = scatter_rows(lambda owner: dot(pick(mixed_turned, owner, rows, 0), out_slice_full))
    attn_normed, inverse_two = norm_forward(attended, gains[:, 1])
    hidden = inputs + attn_normed
    ffn_normed, inverse_three = norm_forward(hidden, gains[:, 2])
    ffn_turned = dot(ffn_normed.astype(BF16), wide_order).astype(BF16)
    ffn_all = gather_rows(ffn_turned)

    gate_up = dot(ffn_all, geglu_full)
    gate, upper = gate_up[:, :ff_slice], gate_up[:, ff_slice:]
    product = (jax.nn.gelu(gate, approximate=True) * upper).astype(BF16)

    def branch_columns(weight):
        def part_of(owner):
            return dot(pick(product, owner, rows, 0), weight)

        return scatter_rows(part_of)

    branch_late = branch_columns(down_late)
    branch = jnp.concatenate([branch_columns(down_early), branch_late], axis=1)
    branch_normed, inverse_four = norm_forward(branch, gains[:, 3])
    query_pos = seq_index * rows + jnp.arange(rows, dtype=jnp.int32)
    live_rows = (query_pos < seq_lengths[0]).astype(F32)[:, None]
    layer_out = ((hidden + branch_normed) * live_rows).astype(BF16)
    row_rms = jnp.sqrt(jnp.mean(inputs * inputs, axis=-1) + EPSILON)

    upstream = upstream * live_rows
    grad_branch, gain_four = norm_backward(branch, inverse_four, gains[:, 3], upstream)
    branch_low = grad_branch.astype(BF16)
    branch_alls = [gather_rows(branch_low[:, part]) for part in parts]
    down_terms = []
    for value in branch_alls:
        down_terms.append(dot_tn(product, value).astype(BF16))
    down_sums = [collect(term) for term in down_terms]
    branch_alls = after(branch_alls, down_terms)
    grad_product = dot_nt(branch_alls[0], down_early) + dot_nt(branch_alls[1], down_late)
    activated, gelu_pull = jax.vjp(lambda value: jax.nn.gelu(value, approximate=True), gate)
    grad_gate = gelu_pull(grad_product * upper)[0]
    grad_upper = grad_product * activated
    gate_up_grad = jnp.concatenate([grad_gate, grad_upper], axis=1).astype(BF16)
    geglu_term = dot_tn(ffn_all, gate_up_grad).astype(BF16)
    geglu_sums = collect(geglu_term)
    (gate_up_grad,) = after([gate_up_grad], [geglu_term])
    ffn_total = dot_nt(gate_up_grad, geglu_full)

    def ffn_part(owner):
        return pick(ffn_total, owner, rows, 0)

    grad_ffn = dot_nt(scatter_rows(ffn_part).astype(BF16), wide_order)
    grad_hidden_norm, gain_three = norm_backward(hidden, inverse_three, gains[:, 2], grad_ffn)
    grad_hidden = upstream + grad_hidden_norm
    grad_attended, gain_two = norm_backward(attended, inverse_two, gains[:, 1], grad_hidden)
    attended_all = gather_rows(grad_attended.astype(BF16))
    grad_mixed_turned = dot_nt(attended_all, out_slice_full).astype(BF16)
    grad_mixed = dot_nt(grad_mixed_turned, head_order).astype(BF16)
    out_term = dot_tn(mixed_turned, attended_all).astype(BF16)
    out_blocks = jnp.transpose(
        out_term.reshape(-1, heads, share, d_groups, BLK), (0, 3, 2, 1, 4)
    ).reshape(D, query_slice)
    (grad_mixed, out_blocks) = after([grad_mixed, out_blocks], [])
    grad_merged = attention_backward(merged, grad_mixed, seq_lengths, prefix_lengths, heads)
    qkv_term = dot_tn(normed_all, grad_merged).astype(BF16)
    heads_sums = collect(jnp.concatenate([qkv_term, out_blocks], axis=1))
    grad_normed = dot_nt(
        scatter_rows(lambda owner: dot_nt(pick(grad_merged, owner, rows, 0), qkv_slice_full)).astype(BF16),
        wide_order,
    )
    grad_input_norm, gain_one = norm_backward(inputs, inverse_one, gains[:, 0], grad_normed)
    token_grad = grad_hidden + grad_input_norm

    turned = jnp.concatenate(
        [
            geglu_sums[turn][:, side * ff_slice : (side + 1) * ff_slice]
            for turn in range(seq_count)
            for side in range(2)
        ],
        axis=0,
    )
    geglu_natural = dot_nt(turned, wide_order).astype(BF16)
    geglu_natural = geglu_natural.reshape(
        seq_count, 2, d_groups, share, ff_slice
    )
    heads_local = [value.reshape(d_groups, share, -1) for value in heads_sums]
    down_local = [
        jnp.concatenate([early, late], axis=1).reshape(d_groups, share, D)
        for early, late in zip(*down_sums)
    ]

    def in_order(items):
        return assemble([item[None] for item in items])

    qkv_slices = in_order(heads_local)
    out_grad = (
        jnp.transpose(
            qkv_slices[..., qkv_slice:].reshape(seq_count, d_groups, share, heads, BLK),
            (2, 0, 3, 1, 4),
        )
        .reshape(share, QUERY_FEATURES // BLK, D)
        .astype(F32)
    )
    down_grad = jnp.transpose(in_order(down_local).reshape(FF // BLK, share, D), (1, 0, 2)).astype(F32)

    def columns(value):
        return jnp.transpose(value, (2, 1, 0, 3)).reshape(share, d_groups, -1)

    qkv_grad = jnp.concatenate(
        [
            columns(qkv_slices[..., :query_slice]),
            columns(qkv_slices[..., query_slice : query_slice + key_slice]),
            columns(qkv_slices[..., query_slice + key_slice : qkv_slice]),
        ],
        axis=-1,
    ).astype(F32)
    geglu_slices = in_order([geglu_natural[turn] for turn in range(seq_count)])
    geglu_grad = jnp.transpose(geglu_slices, (3, 2, 1, 0, 4)).reshape(share, d_groups, 2 * FF).astype(F32)

    devices = lax.axis_size(ALL)
    capacity = first_moment.shape[0]
    early = capacity * 3 // 8 * 2
    sizes = (early, capacity - early + 1)
    number = jnp.arange(block_owners.shape[0], dtype=jnp.int32)
    same = (block_owners[:, None] == block_owners[None, :]) & (number[None, :] < number[:, None])
    rank = jnp.sum(same.astype(jnp.int32), axis=1)
    slots = jnp.where(
        rank < early,
        block_owners * early + rank,
        devices * early + block_owners * sizes[1] + rank - early,
    )

    gain_term = jnp.stack([gain_one, gain_two, gain_three, gain_four], axis=1)
    gain_share = D // devices
    gain_flat = gain_term.reshape(devices, gain_share * 4)
    gain_high = gain_flat.astype(BF16)
    gain_low = (gain_flat - gain_high.astype(F32)).astype(BF16)
    room = share * BLK
    gain_pair = jnp.concatenate([gain_high, gain_low], axis=1)
    extra = jnp.pad(gain_pair, ((0, 0), (0, room - gain_pair.shape[1]))).reshape(devices, share, BLK)

    ff_blocks = ff_slice // BLK
    out_base = d_groups * (QUERY_FEATURES + 2 * KEY_FEATURES) // BLK
    geglu_base = out_base + (QUERY_FEATURES // BLK) * (D // BLK)
    down_base = geglu_base + d_groups * 2 * FF // BLK
    if share % 8 == 0:
        pieces, layout = [], []
        query_blocks, key_blocks = query_slice // BLK, key_slice // BLK
        wide = (QUERY_FEATURES + 2 * KEY_FEATURES) // BLK
        d_blocks = D // BLK
        for turn in range(seq_count):
            qkv_columns = [(at, at, query_blocks, 0) for at in range(query_blocks)]
            for kind, begin in enumerate((QUERY_FEATURES, QUERY_FEATURES + KEY_FEATURES)):
                qkv_columns += [
                    (query_blocks + kind * key_blocks + at, begin // BLK + at, key_blocks, 0)
                    for at in range(key_blocks)
                ]
            out_columns = [
                (qkv_slice // BLK + at, at * d_blocks, heads * d_blocks, 0) for at in range(heads)
            ]
            layout.append((len(pieces), turn, 0, wide, qkv_columns))
            layout.append((len(pieces), turn, out_base, 1, out_columns))
            pieces.append(heads_local[turn])
            for side in range(2):
                side_columns = [
                    (at, side * FF // BLK + at, ff_blocks, 0) for at in range(ff_blocks)
                ]
                layout.append((len(pieces), turn, geglu_base, 2 * FF // BLK, side_columns))
                pieces.append(geglu_natural[turn, side])
            down_columns = [(at, at, 0, d_groups) for at in range(d_blocks)]
            layout.append((len(pieces), turn, down_base, d_blocks, down_columns))
            pieces.append(down_local[turn])
        outgoing = place_pieces(pieces, extra, slots, seq_index, layout, devices, sizes)
    else:

        def to_pieces(gradient):
            count_of_rows, groups, col_count = gradient.shape
            shaped = gradient.astype(BF16).reshape(count_of_rows, groups, col_count // BLK, BLK)
            return jnp.transpose(shaped, (1, 2, 0, 3)).reshape(-1, count_of_rows, BLK)

        every = jnp.concatenate(
            [to_pieces(qkv_grad), to_pieces(out_grad), to_pieces(geglu_grad), to_pieces(down_grad)],
            axis=0,
        )
        split = devices * early
        flat = jnp.zeros((devices * sum(sizes), share, BLK), BF16).at[slots].set(every)
        flat = flat.at[split + (jnp.arange(devices) + 1) * sizes[1] - 1].set(extra)
        outgoing = (flat[:split], flat[split:])

    def exchange(value):
        moved = lax.all_to_all(value, ALL, split_axis=0, concat_axis=0, tiled=True)
        return moved.reshape(devices, -1, share, BLK)

    def blocks_of(value, count):
        if share % 8 == 0:
            return value
        return jnp.transpose(value[:, :count], (1, 0, 2, 3)).reshape(count, BLK, BLK)

    incoming_one = exchange(outgoing[0])
    later, incoming_one = lax.optimization_barrier((outgoing[1], incoming_one))
    incoming_two = exchange(later)
    gain_parts = incoming_two[:, sizes[1] - 1].reshape(devices, room)[:, : 2 * gain_share * 4]
    gain_sums = jnp.sum(gain_parts.astype(F32), axis=0)
    gains_grad = (gain_sums[: gain_share * 4] + gain_sums[gain_share * 4 :]).reshape(gain_share, 4)
    state = (first_moment, second_moment, left_basis, right_basis, slot_weight)
    updated = soap(blocks_of(incoming_one, early), state, 0, early, ())
    first_new, second_new, weight_new = soap(
        blocks_of(incoming_two, capacity - early), state, early, capacity - early, updated
    )
    return (
        layer_out[None],
        row_rms[None],
        token_grad[None],
        qkv_grad,
        out_grad,
        geglu_grad,
        down_grad,
        gains_grad,
        first_new,
        second_new,
        weight_new,
    )


def solution(mesh):
    in_specs = (
        P("dp", "seq", None),
        P("dp", "seq", None),
        P(ALL, None, None),
        P(ALL, None, None),
        P(ALL, None, None),
        P(ALL, None, None),
        P(ALL, None),
        P("dp"),
        P("dp"),
        P(),
        P(ALL, None, None),
        P(ALL, None, None),
        P(ALL, None, None),
        P(ALL, None, None),
        P(ALL, None, None),
    )
    out_specs = (
        P("dp", "seq", None),
        P("dp", "seq"),
        P("dp", "seq", None),
        P(ALL, None, None),
        P(ALL, None, None),
        P(ALL, None, None),
        P(ALL, None, None),
        P(ALL, None),
        P(ALL, None, None),
        P(ALL, None, None),
        P(ALL, None, None),
    )

    return jax.shard_map(body, mesh=mesh, in_specs=in_specs, out_specs=out_specs, check_vma=False)
```

```python
import functools

import jax
import jax.numpy as jnp
from jax import lax
from jax.experimental import pallas as pl
from jax.experimental.layout import Layout, with_layout_constraint
from jax.experimental.pallas import tpu as pltpu
from jax.sharding import PartitionSpec as P


D = 2304
QUERY_HEADS = 8
HEAD_SIZE = 256
FF = 9216
BLK = 256
QUERY_FEATURES = 2048
KEY_FEATURES = 1024


EPSILON = 1e-06
SOFT_CAP = 50.0
NEGATIVE = -1e30
BETA_ONE = 0.9
BETA_TWO = 0.95
STEP_RATE = 0.05
TINY_ADD = 1e-08
CLIP_NORM = 1.0


F32 = jnp.float32
BF16 = jnp.bfloat16
ALL = ("seq", "dp")


def norm_forward(value_rows, gain):
    inverse = lax.rsqrt(jnp.mean(value_rows * value_rows, axis=-1, keepdims=True) + EPSILON)
    return (value_rows * inverse * gain, inverse)


def norm_backward(value_rows, inverse, gain, upstream):
    weighted = upstream * gain
    cubed = inverse * inverse * inverse
    grad_in = inverse * weighted - value_rows * cubed * jnp.mean(
        value_rows * weighted, axis=-1, keepdims=True
    )
    return (grad_in, jnp.sum(upstream * value_rows * inverse, axis=0))


def dot(left, right):
    return jnp.dot(left, right, preferred_element_type=F32)


def dot_nt(left, right):
    return lax.dot_general(left, right, (((1,), (1,)), ((), ())), preferred_element_type=F32)


def dot_tn(left, right):
    return lax.dot_general(left, right, (((0,), (0,)), ((), ())), preferred_element_type=F32)


def block_probs(query, keys, row_start, length, prefix):
    raw = dot_nt(query, keys)
    bent = jnp.tanh(raw * (HEAD_SIZE ** (-0.5) / SOFT_CAP))
    key_pos = lax.broadcasted_iota(jnp.int32, raw.shape, 1)
    query_pos = row_start + lax.broadcasted_iota(jnp.int32, raw.shape, 0)
    visible = (key_pos < length) & ((key_pos <= query_pos) | (key_pos < prefix))
    capped = jnp.where(visible, SOFT_CAP * bent, NEGATIVE)
    exponent = jnp.exp(capped - jnp.max(capped, axis=-1, keepdims=True))
    prob = exponent / jnp.sum(exponent, axis=-1, keepdims=True)
    return (prob, bent)


def attention_forward_kernel(heads, length_ref, prefix_ref, merged_ref, mixed_ref):
    length, prefix = length_ref[0], prefix_ref[0]
    key_col, value_col = heads * HEAD_SIZE, (heads + 1) * HEAD_SIZE
    tokens = merged_ref.shape[0]
    for head in range(heads):
        for start in range(0, tokens, BLK):
            rows, width = slice(start, start + BLK), start + BLK
            head_cols = slice(head * HEAD_SIZE, (head + 1) * HEAD_SIZE)
            keys = merged_ref[:width, key_col : key_col + HEAD_SIZE]
            values = merged_ref[:width, value_col : value_col + HEAD_SIZE]
            prob, _ = block_probs(merged_ref[rows, head_cols], keys, start, length, prefix)
            mixed_ref[rows, head_cols] = dot(prob.astype(BF16), values).astype(BF16)


def attention_backward_kernel(
    heads, length_ref, prefix_ref, merged_ref, upstream_ref, grad_ref, keys_acc, values_acc
):
    length, prefix = length_ref[0], prefix_ref[0]
    key_col, value_col = heads * HEAD_SIZE, (heads + 1) * HEAD_SIZE
    tokens = merged_ref.shape[0]
    keys_acc[...] = jnp.zeros_like(keys_acc)
    values_acc[...] = jnp.zeros_like(values_acc)
    for head in range(heads):
        for start in range(0, tokens, BLK):
            rows, width = slice(start, start + BLK), start + BLK
            head_cols = slice(head * HEAD_SIZE, (head + 1) * HEAD_SIZE)
            query = merged_ref[rows, head_cols]
            keys = merged_ref[:width, key_col : key_col + HEAD_SIZE]
            values = merged_ref[:width, value_col : value_col + HEAD_SIZE]
            upstream = upstream_ref[rows, head_cols]
            prob, bent = block_probs(query, keys, start, length, prefix)
            grad_prob = dot_nt(upstream, values)
            balance = jnp.sum(prob * grad_prob, axis=-1, keepdims=True)
            grad_raw = (
                prob * (grad_prob - balance) * (1.0 - bent * bent) * HEAD_SIZE ** (-0.5)
            ).astype(BF16)
            grad_ref[rows, head_cols] = dot(grad_raw, keys).astype(BF16)
            keys_acc[:width, :] += dot_tn(grad_raw, query)
            values_acc[:width, :] += dot_tn(prob.astype(BF16), upstream)
    grad_ref[:, key_col : key_col + HEAD_SIZE] = keys_acc[...].astype(BF16)
    grad_ref[:, value_col : value_col + HEAD_SIZE] = values_acc[...].astype(BF16)


SMEM_SPEC = pl.BlockSpec(memory_space=pltpu.SMEM)
VMEM_SPEC = pl.BlockSpec(memory_space=pltpu.VMEM)


def attention_forward(merged, length, prefix, heads):
    tokens = merged.shape[0]
    flops = 4 * heads * tokens * tokens * HEAD_SIZE
    return pl.pallas_call(
        functools.partial(attention_forward_kernel, heads),
        out_shape=jax.ShapeDtypeStruct((tokens, heads * HEAD_SIZE), BF16),
        in_specs=[SMEM_SPEC, SMEM_SPEC, VMEM_SPEC],
        out_specs=VMEM_SPEC,
        compiler_params=pltpu.CompilerParams(vmem_limit_bytes=40 << 20),
        cost_estimate=pl.CostEstimate(
            flops=flops, bytes_accessed=4 << 20, transcendentals=2 * heads * tokens * tokens
        ),
    )(length, prefix, merged)


def attention_backward(merged, upstream, length, prefix, heads):
    tokens = merged.shape[0]
    flops = 10 * heads * tokens * tokens * HEAD_SIZE
    return pl.pallas_call(
        functools.partial(attention_backward_kernel, heads),
        out_shape=jax.ShapeDtypeStruct(merged.shape, BF16),
        in_specs=[SMEM_SPEC, SMEM_SPEC, VMEM_SPEC, VMEM_SPEC],
        out_specs=VMEM_SPEC,
        scratch_shapes=[pltpu.VMEM((tokens, HEAD_SIZE), F32), pltpu.VMEM((tokens, HEAD_SIZE), F32)],
        compiler_params=pltpu.CompilerParams(vmem_limit_bytes=48 << 20),
        cost_estimate=pl.CostEstimate(
            flops=flops, bytes_accessed=6 << 20, transcendentals=2 * heads * tokens * tokens
        ),
    )(length, prefix, merged, upstream)


def place_kernel(layout, devices, sizes, slots_ref, *refs):
    count = len(refs) - 4
    pieces, extra, out_one, out_two, flat = refs[:count], refs[count], *refs[count + 1 :]
    flat[...] = jnp.zeros_like(flat)
    split = devices * sizes[0]

    @pl.loop(0, devices)
    def _(at):
        flat[split + (at + 1) * sizes[1] - 1] = extra[at]

    seq_index = slots_ref[slots_ref.shape[0] - 1]
    for index, turn, base, per_row, columns in layout:
        piece = pieces[index]
        source = jnp.bitwise_xor(seq_index, turn)

        @pl.loop(0, piece.shape[0])
        def _(a, piece=piece, base=base, per_row=per_row, columns=columns, source=source):
            for local, fixed, factor, row_factor in columns:
                block = base + (a + source * row_factor) * per_row + fixed + source * factor
                flat[slots_ref[block]] = piece[a, :, local * BLK : (local + 1) * BLK]

    out_one[...] = flat[:split]
    out_two[...] = flat[split:]


def place_pieces(pieces, extra, slots, seq_index, layout, devices, sizes):
    share = extra.shape[1]
    table = jnp.concatenate([slots, seq_index[None]]).astype(jnp.int32)
    return pl.pallas_call(
        functools.partial(place_kernel, layout, devices, sizes),
        out_shape=tuple(jax.ShapeDtypeStruct((devices * size, share, BLK), BF16) for size in sizes),
        in_specs=[SMEM_SPEC] + [VMEM_SPEC] * (len(pieces) + 1),
        out_specs=(VMEM_SPEC, VMEM_SPEC),
        scratch_shapes=[pltpu.VMEM((devices * sum(sizes), share, BLK), BF16)],
        compiler_params=pltpu.CompilerParams(vmem_limit_bytes=48 << 20),
        cost_estimate=pl.CostEstimate(flops=0, bytes_accessed=12 << 20, transcendentals=0),
    )(table, *pieces, extra)


def soap_kernel(group, incoming, first, second, left, right, master, *outs):
    first_out, second_out, weight_out = outs[-3:]
    for at in range(group):
        if len(incoming.shape) == 4:
            grad = incoming[:, at].astype(F32).reshape(BLK, BLK)
        else:
            grad = incoming[at].astype(F32)
        size = jnp.sqrt(jnp.sum(grad * grad))
        scale = CLIP_NORM / jnp.maximum(size, CLIP_NORM)
        left_low = left[at].astype(BF16)
        right_low = right[at].astype(BF16)
        turned = dot_tn(left_low, grad.astype(BF16)).astype(BF16)
        rotated = dot(turned, right_low) * scale
        first_new = BETA_ONE * first[at] + (1.0 - BETA_ONE) * rotated
        second_new = BETA_TWO * second[at] + (1.0 - BETA_TWO) * rotated * rotated
        first_out[at] = first_new
        second_out[at] = second_new
        direction = (first_new / (jnp.sqrt(second_new) + TINY_ADD)).astype(BF16)
        back_left = dot(left_low, direction).astype(BF16)
        weight_out[at] = master[at] - STEP_RATE * dot_nt(back_left, right_low)


def soap(incoming, state, begin, count, earlier):
    capacity = state[0].shape[0]
    group = 2 if begin % 2 == 0 and count % 2 == 0 else 1
    spec = pl.BlockSpec((group, BLK, BLK), lambda at: (at + begin // group, 0, 0))
    if incoming.ndim == 4:
        grad_spec = pl.BlockSpec(
            (incoming.shape[0], group) + incoming.shape[2:], lambda at: (0, at, 0, 0)
        )
    else:
        grad_spec = pl.BlockSpec((group, BLK, BLK), lambda at: (at, 0, 0))
    shape = jax.ShapeDtypeStruct((capacity, BLK, BLK), F32)
    return pl.pallas_call(
        functools.partial(soap_kernel, group),
        grid=(count // group,),
        out_shape=(shape, shape, shape),
        in_specs=[grad_spec] + [spec] * 5 + [pl.BlockSpec(memory_space=pl.ANY)] * len(earlier),
        out_specs=(spec, spec, spec),
        input_output_aliases={6 + at: at for at in range(len(earlier))},
        compiler_params=pltpu.CompilerParams(vmem_limit_bytes=48 << 20),
        cost_estimate=pl.CostEstimate(
            flops=8 * count * BLK**3,
            bytes_accessed=34 * count * BLK * BLK,
            transcendentals=2 * count * BLK * BLK,
        ),
    )(incoming, *state, *earlier)


def body(
    tokens,
    cotangent,
    qkv_weight,
    out_weight,
    geglu_weight,
    down_weight,
    norm_gains,
    seq_lengths,
    prefix_lengths,
    block_owners,
    first_moment,
    second_moment,
    left_basis,
    right_basis,
    slot_weight,
):
    inputs = tokens[0].astype(F32)
    upstream = cotangent[0].astype(F32)
    rows = inputs.shape[0]
    seq_count = lax.axis_size("seq")
    dp_count = lax.axis_size("dp")
    seq_index = lax.axis_index("seq")
    share = qkv_weight.shape[0]
    heads = QUERY_HEADS // seq_count
    query_slice = heads * HEAD_SIZE
    key_slice = KEY_FEATURES // seq_count
    ff_slice = FF // seq_count
    d_groups = D // BLK
    cut = D * 5 // 18
    parts = (slice(0, cut), slice(cut, D))
    qkv_slice = query_slice + 2 * key_slice

    def swap(value, turn):
        return lax.ppermute(value, "seq", [(at, at ^ turn) for at in range(seq_count)])

    def double_gather(value):
        for axis, size in (("dp", dp_count), ("seq", seq_count)):
            step = 1
            while step < size:
                other = lax.ppermute(value, axis, [(at, at ^ step) for at in range(size)])
                upper = (lax.axis_index(axis) & step) != 0
                value = jnp.concatenate(
                    [jnp.where(upper, other, value), jnp.where(upper, value, other)], axis=0
                )
                step *= 2
        return value

    def owner_of(turn):
        return jnp.bitwise_xor(seq_index, turn)

    def pick(value, index, size, axis):
        return lax.dynamic_slice_in_dim(value, index * size, size, axis)

    def assemble(items):
        size = items[0].shape[0]
        buffer = jnp.zeros((size * seq_count,) + items[0].shape[1:], items[0].dtype)
        for turn, item in enumerate(items):
            start = (owner_of(turn) * size,) + (0,) * (item.ndim - 1)
            buffer = lax.dynamic_update_slice(buffer, item, start)
        return buffer

    def gather_rows(value):
        received = {turn: swap(value, turn) for turn in range(seq_count - 1, 0, -1)}
        return assemble([value] + [received[turn] for turn in range(1, seq_count)])

    def scatter_rows(part_of, own_part_of=None):
        received = []
        for turn in range(seq_count - 1, 0, -1):
            part = part_of(owner_of(turn)).astype(BF16)
            received.append(swap(part, turn))
        result = (own_part_of or part_of)(seq_index)
        for value in received:
            result = result + value.astype(F32)
        return result

    def spread(piece_for):
        received = [piece_for(seq_index)]
        for turn in range(1, seq_count):
            received.append(swap(piece_for(owner_of(turn)), turn))
        operand = assemble(received)
        return lax.all_gather(operand, "dp", axis=0, tiled=True)

    def collect(gradient):
        summed = lax.psum_scatter(gradient, "dp", scatter_dimension=0, tiled=True)
        size = summed.shape[0] // seq_count
        result = [pick(summed, seq_index, size, 0)]
        for turn in range(1, seq_count):
            result.append(swap(pick(summed, owner_of(turn), size, 0), turn))
        return result

    def after(values, others):
        return list(lax.optimization_barrier(tuple(values) + tuple(others)))[: len(values)]

    def row_order(groups):
        at = jnp.arange(groups * BLK, dtype=jnp.int32)
        inner = at % share
        group = (at // share) % groups
        device = at // (share * groups)
        natural = share * (dp_count * (device % seq_count) + device // seq_count) + inner
        return group * BLK + natural

    def order_matrix(groups):
        return (jnp.arange(groups * BLK, dtype=jnp.int32)[:, None] == row_order(groups)[None, :]).astype(BF16)

    wide_order = order_matrix(d_groups)
    head_order = order_matrix(heads)

    def local_rows(weight):
        return jnp.transpose(weight.astype(BF16), (1, 0, 2))

    qkv_low = local_rows(qkv_weight).reshape(d_groups * share, -1)
    out_low = local_rows(out_weight)
    down_low = local_rows(down_weight)
    gain_full = double_gather(norm_gains.astype(BF16).reshape(1, -1)).reshape(D, 4)

    def out_piece(target):
        piece = pick(out_low, target, heads, 0).reshape(heads, share, d_groups, BLK)
        return jnp.transpose(piece, (2, 1, 0, 3)).reshape(d_groups * share, query_slice)

    def qkv_piece(target):
        return jnp.concatenate(
            [
                pick(qkv_low[:, :QUERY_FEATURES], target, query_slice, 1),
                pick(qkv_low[:, QUERY_FEATURES : QUERY_FEATURES + KEY_FEATURES], target, key_slice, 1),
                pick(qkv_low[:, QUERY_FEATURES + KEY_FEATURES :], target, key_slice, 1),
                out_piece(target),
            ],
            axis=1,
        )

    def down_piece(part):
        return lambda target: pick(down_low[..., part], target, d_groups, 0).reshape(
            d_groups * share, -1
        )

    heads_full = spread(qkv_piece)
    qkv_slice_full = heads_full[:, :qkv_slice]
    out_slice_full = jnp.transpose(
        heads_full[:, qkv_slice:].reshape(-1, d_groups, share, heads, BLK), (0, 3, 2, 1, 4)
    ).reshape(query_slice, D)

    geglu_rows = jnp.transpose(
        geglu_weight.astype(BF16).reshape(share, d_groups, 2 * seq_count, ff_slice), (2, 1, 0, 3)
    ).reshape(2 * seq_count * d_groups * share, ff_slice)
    geglu_turned = dot(geglu_rows, wide_order).astype(BF16).reshape(
        2 * seq_count, d_groups * share, ff_slice
    )

    def geglu_piece(target):
        return jnp.concatenate(
            [
                lax.dynamic_index_in_dim(geglu_turned, target, 0, False),
                lax.dynamic_index_in_dim(geglu_turned, target + seq_count, 0, False),
            ],
            axis=1,
        )

    geglu_full = spread(geglu_piece)
    down_late = spread(down_piece(parts[1]))
    down_early = spread(down_piece(parts[0]))

    gains = gain_full.astype(F32)
    normed, inverse_one = norm_forward(inputs, gains[:, 0])
    normed_turned = dot(normed.astype(BF16), wide_order).astype(BF16)
    normed_all = gather_rows(normed_turned)
    merged = dot(normed_all, qkv_slice_full).astype(BF16)
    mixed = attention_forward(merged, seq_lengths, prefix_lengths, heads)
    mixed_turned = dot(mixed, head_order).astype(BF16)
    attended = scatter_rows(lambda owner: dot(pick(mixed_turned, owner, rows, 0), out_slice_full))
    attn_normed, inverse_two = norm_forward(attended, gains[:, 1])
    hidden = inputs + attn_normed
    ffn_normed, inverse_three = norm_forward(hidden, gains[:, 2])
    ffn_turned = dot(ffn_normed.astype(BF16), wide_order).astype(BF16)
    ffn_all = gather_rows(ffn_turned)

    gate_up = dot(ffn_all, geglu_full)
    gate, upper = gate_up[:, :ff_slice], gate_up[:, ff_slice:]
    product = (jax.nn.gelu(gate, approximate=True) * upper).astype(BF16)

    def branch_columns(weight):
        def part_named():
            def part_of(owner):
                return dot(pick(product, owner, rows, 0), weight)

            return part_of

        own_part_of = part_named()
        return scatter_rows(
            part_named(), lambda owner: lax.optimization_barrier(own_part_of(owner))
        )

    branch_late = branch_columns(down_late)
    branch = jnp.concatenate([branch_columns(down_early), branch_late], axis=1)
    branch_normed, inverse_four = norm_forward(branch, gains[:, 3])
    query_pos = seq_index * rows + jnp.arange(rows, dtype=jnp.int32)
    live_rows = (query_pos < seq_lengths[0]).astype(F32)[:, None]
    layer_out = ((hidden + branch_normed) * live_rows).astype(BF16)
    row_rms = jnp.sqrt(jnp.mean(inputs * inputs, axis=-1) + EPSILON)

    upstream = upstream * live_rows
    grad_branch, gain_four = norm_backward(branch, inverse_four, gains[:, 3], upstream)
    branch_low = grad_branch.astype(BF16)
    branch_alls = [gather_rows(branch_low[:, part]) for part in parts]
    down_terms = []
    for value in branch_alls:
        down_terms.append(dot_tn(product, value).astype(BF16))
    down_sums = [collect(term) for term in down_terms]
    branch_alls = after(branch_alls, down_terms)
    grad_product = dot_nt(branch_alls[0], down_early) + dot_nt(branch_alls[1], down_late)
    activated, gelu_pull = jax.vjp(lambda value: jax.nn.gelu(value, approximate=True), gate)
    grad_gate = gelu_pull(grad_product * upper)[0]
    grad_upper = grad_product * activated
    gate_up_grad = jnp.concatenate([grad_gate, grad_upper], axis=1).astype(BF16)
    geglu_term = dot_tn(ffn_all, gate_up_grad).astype(BF16)
    geglu_sums = collect(geglu_term)
    ffn_total = dot_nt(gate_up_grad, geglu_full)

    def ffn_part(owner):
        return pick(ffn_total, owner, rows, 0)

    grad_ffn = dot_nt(scatter_rows(ffn_part).astype(BF16), wide_order)
    grad_hidden_norm, gain_three = norm_backward(hidden, inverse_three, gains[:, 2], grad_ffn)
    grad_hidden = upstream + grad_hidden_norm
    grad_attended, gain_two = norm_backward(attended, inverse_two, gains[:, 1], grad_hidden)
    attended_all = gather_rows(grad_attended.astype(BF16))
    grad_mixed_turned = dot_nt(attended_all, out_slice_full).astype(BF16)
    grad_mixed = dot_nt(grad_mixed_turned, head_order).astype(BF16)
    out_term = dot_tn(mixed_turned, attended_all).astype(BF16)
    out_blocks = jnp.transpose(
        out_term.reshape(-1, heads, share, d_groups, BLK), (0, 3, 2, 1, 4)
    ).reshape(D, query_slice)
    out_blocks = with_layout_constraint(out_blocks, Layout((0, 1)))
    grad_merged = attention_backward(merged, grad_mixed, seq_lengths, prefix_lengths, heads)
    qkv_term = dot_tn(normed_all, grad_merged).astype(BF16)
    qkv_term = with_layout_constraint(qkv_term, Layout((0, 1)))
    heads_sums = collect(jnp.concatenate([qkv_term, out_blocks], axis=1))
    (sent_merged,) = after([grad_merged], down_sums[0] + down_sums[1])
    (own_merged,) = after([grad_merged], geglu_sums)
    grad_normed = scatter_rows(
        lambda owner: dot_nt(pick(sent_merged, owner, rows, 0), qkv_slice_full),
        lambda owner: dot_nt(pick(own_merged, owner, rows, 0), qkv_slice_full),
    )
    grad_normed = dot_nt(grad_normed.astype(BF16), wide_order)
    grad_input_norm, gain_one = norm_backward(inputs, inverse_one, gains[:, 0], grad_normed)
    token_grad = grad_hidden + grad_input_norm

    turned = jnp.concatenate(
        [
            geglu_sums[turn][:, side * ff_slice : (side + 1) * ff_slice]
            for turn in range(seq_count)
            for side in range(2)
        ],
        axis=0,
    )
    geglu_natural = dot_nt(turned, wide_order).astype(BF16)
    geglu_natural = geglu_natural.reshape(
        seq_count, 2, d_groups, share, ff_slice
    )
    heads_local = [value.reshape(d_groups, share, -1) for value in heads_sums]
    down_local = [
        jnp.concatenate([early, late], axis=1).reshape(d_groups, share, D)
        for early, late in zip(*down_sums)
    ]

    def in_order(items):
        return assemble([item[None] for item in items])

    qkv_slices = in_order(heads_local)
    out_grad = (
        jnp.transpose(
            qkv_slices[..., qkv_slice:].reshape(seq_count, d_groups, share, heads, BLK),
            (2, 0, 3, 1, 4),
        )
        .reshape(share, QUERY_FEATURES // BLK, D)
        .astype(F32)
    )
    down_grad = jnp.transpose(in_order(down_local).reshape(FF // BLK, share, D), (1, 0, 2)).astype(F32)

    def columns(value):
        return jnp.transpose(value, (2, 1, 0, 3)).reshape(share, d_groups, -1)

    qkv_grad = jnp.concatenate(
        [
            columns(qkv_slices[..., :query_slice]),
            columns(qkv_slices[..., query_slice : query_slice + key_slice]),
            columns(qkv_slices[..., query_slice + key_slice : qkv_slice]),
        ],
        axis=-1,
    ).astype(F32)
    geglu_slices = in_order([geglu_natural[turn] for turn in range(seq_count)])
    geglu_grad = jnp.transpose(geglu_slices, (3, 2, 1, 0, 4)).reshape(share, d_groups, 2 * FF).astype(F32)

    devices = lax.axis_size(ALL)
    capacity = first_moment.shape[0]
    early = capacity * 3 // 8 * 2
    sizes = (early, capacity - early + 1)
    number = jnp.arange(block_owners.shape[0], dtype=jnp.int32)
    same = (block_owners[:, None] == block_owners[None, :]) & (number[None, :] < number[:, None])
    rank = jnp.sum(same.astype(jnp.int32), axis=1)
    slots = jnp.where(
        rank < early,
        block_owners * early + rank,
        devices * early + block_owners * sizes[1] + rank - early,
    )

    gain_term = jnp.stack([gain_one, gain_two, gain_three, gain_four], axis=1)
    gain_share = D // devices
    gain_flat = gain_term.reshape(devices, gain_share * 4)
    gain_high = gain_flat.astype(BF16)
    gain_low = (gain_flat - gain_high.astype(F32)).astype(BF16)
    room = share * BLK
    gain_pair = jnp.concatenate([gain_high, gain_low], axis=1)
    extra = jnp.pad(gain_pair, ((0, 0), (0, room - gain_pair.shape[1]))).reshape(devices, share, BLK)

    ff_blocks = ff_slice // BLK
    out_base = d_groups * (QUERY_FEATURES + 2 * KEY_FEATURES) // BLK
    geglu_base = out_base + (QUERY_FEATURES // BLK) * (D // BLK)
    down_base = geglu_base + d_groups * 2 * FF // BLK
    if share % 8 == 0:
        pieces, layout = [], []
        query_blocks, key_blocks = query_slice // BLK, key_slice // BLK
        wide = (QUERY_FEATURES + 2 * KEY_FEATURES) // BLK
        d_blocks = D // BLK
        for turn in range(seq_count):
            qkv_columns = [(at, at, query_blocks, 0) for at in range(query_blocks)]
            for kind, begin in enumerate((QUERY_FEATURES, QUERY_FEATURES + KEY_FEATURES)):
                qkv_columns += [
                    (query_blocks + kind * key_blocks + at, begin // BLK + at, key_blocks, 0)
                    for at in range(key_blocks)
                ]
            out_columns = [
                (qkv_slice // BLK + at, at * d_blocks, heads * d_blocks, 0) for at in range(heads)
            ]
            layout.append((len(pieces), turn, 0, wide, qkv_columns))
            layout.append((len(pieces), turn, out_base, 1, out_columns))
            pieces.append(heads_local[turn])
            for side in range(2):
                side_columns = [
                    (at, side * FF // BLK + at, ff_blocks, 0) for at in range(ff_blocks)
                ]
                layout.append((len(pieces), turn, geglu_base, 2 * FF // BLK, side_columns))
                pieces.append(geglu_natural[turn, side])
            down_columns = [(at, at, 0, d_groups) for at in range(d_blocks)]
            layout.append((len(pieces), turn, down_base, d_blocks, down_columns))
            pieces.append(down_local[turn])
        outgoing = place_pieces(pieces, extra, slots, seq_index, layout, devices, sizes)
    else:

        def to_pieces(gradient):
            count_of_rows, groups, col_count = gradient.shape
            shaped = gradient.astype(BF16).reshape(count_of_rows, groups, col_count // BLK, BLK)
            return jnp.transpose(shaped, (1, 2, 0, 3)).reshape(-1, count_of_rows, BLK)

        every = jnp.concatenate(
            [to_pieces(qkv_grad), to_pieces(out_grad), to_pieces(geglu_grad), to_pieces(down_grad)],
            axis=0,
        )
        split = devices * early
        flat = jnp.zeros((devices * sum(sizes), share, BLK), BF16).at[slots].set(every)
        flat = flat.at[split + (jnp.arange(devices) + 1) * sizes[1] - 1].set(extra)
        outgoing = (flat[:split], flat[split:])

    def exchange(value):
        moved = lax.all_to_all(value, ALL, split_axis=0, concat_axis=0, tiled=True)
        return moved.reshape(devices, -1, share, BLK)

    def blocks_of(value, count):
        if share % 8 == 0:
            return value
        return jnp.transpose(value[:, :count], (1, 0, 2, 3)).reshape(count, BLK, BLK)

    incoming_one = exchange(outgoing[0])
    later, incoming_one = lax.optimization_barrier((outgoing[1], incoming_one))
    incoming_two = exchange(later)
    gain_parts = incoming_two[:, sizes[1] - 1].reshape(devices, room)[:, : 2 * gain_share * 4]
    gain_sums = jnp.sum(gain_parts.astype(F32), axis=0)
    gains_grad = (gain_sums[: gain_share * 4] + gain_sums[gain_share * 4 :]).reshape(gain_share, 4)
    state = (first_moment, second_moment, left_basis, right_basis, slot_weight)
    updated = soap(blocks_of(incoming_one, early), state, 0, early, ())
    first_new, second_new, weight_new = soap(
        blocks_of(incoming_two, capacity - early), state, early, capacity - early, updated
    )
    return (
        layer_out[None],
        row_rms[None],
        token_grad[None],
        qkv_grad,
        out_grad,
        geglu_grad,
        down_grad,
        gains_grad,
        first_new,
        second_new,
        weight_new,
    )


def solution(mesh):
    in_specs = (
        P("dp", "seq", None),
        P("dp", "seq", None),
        P(ALL, None, None),
        P(ALL, None, None),
        P(ALL, None, None),
        P(ALL, None, None),
        P(ALL, None),
        P("dp"),
        P("dp"),
        P(),
        P(ALL, None, None),
        P(ALL, None, None),
        P(ALL, None, None),
        P(ALL, None, None),
        P(ALL, None, None),
    )
    out_specs = (
        P("dp", "seq", None),
        P("dp", "seq"),
        P("dp", "seq", None),
        P(ALL, None, None),
        P(ALL, None, None),
        P(ALL, None, None),
        P(ALL, None, None),
        P(ALL, None),
        P(ALL, None, None),
        P(ALL, None, None),
        P(ALL, None, None),
    )

    return jax.shard_map(body, mesh=mesh, in_specs=in_specs, out_specs=out_specs, check_vma=False)
```
